32 devices in a mesh: shard: 16 (over z, x, core), task: 2 (over y).
Axes of the slice: x: 2, y: 2, z: 4, core: 2. Of those that a mesh axis runs over, the one named last changes fastest.
Arguments:
- task_deltas: bfloat16 [2, 4, 256, 16384], P('task', None, 'shard')
- rank_scores: int32 [2, 4, 256, 16384], P('task', None, 'shard'), may hold values from 0 to 1073741823
- keep_limits: int32 [2, 4, 8], P('task'), may hold values from 268435456 to 805306367
Outputs:
- merged: bfloat16 [4, 256, 16384], P(None, 'shard', 'task')
The draws below stay inside these ranges and needn't reach their ends.
All inputs are finite; a program needn't handle non-finite values.
Results may differ from the reference program's by a relative error of at most 0.0051.
Values may be sent and summed in bfloat16 or wider, within the bound.
A program may use at most 64 MiB of HBM per device.

```python
import math
import jax
import jax.numpy as jnp
from jax import lax

EXPERTS = 8
FF = 16384
LAYERS = 4
ROWS = 32
TASKS = 2


def draw_task_deltas(key, part):
    key_base, key_column, key_row = jax.random.split(key, 3)
    row_total = EXPERTS * ROWS
    shape = (TASKS, LAYERS, row_total, FF)
    rising = 1.0 + 2.0 * jnp.arange(row_total, dtype=jnp.float32) / max(row_total - 1, 1)
    base = jax.random.normal(key_base, shape, jnp.float32)
    column = 0.03 * jnp.exp(jax.random.uniform(key_column, (TASKS, LAYERS, 1, FF), jnp.float32, 0.0, math.log(10.0)))
    row_scale = jnp.exp(jax.random.uniform(key_row, (TASKS, LAYERS, row_total, 1), jnp.float32, 0.0, math.log(10.0)))
    return (base * column * row_scale * rising[None, None, :, None]).astype(jnp.bfloat16)


def plant(result, stream_key, smallest, top_value):
    longest = result.shape.index(max(result.shape))
    spots = []
    for shift in (0, 1):
        where = [jax.random.randint(jax.random.fold_in(stream_key, axis), (), 0, length) for axis, length in enumerate(result.shape)]
        where[longest] = (where[longest] + shift) % result.shape[longest]
        spots.append(tuple(where))
    return result.at[spots[0]].set(smallest).at[spots[1]].set(top_value)


def setup_inputs(seed: int = 0) -> dict:
    key_list = jax.random.split(jax.random.key(seed), 4)
    return {
        "task_deltas": draw_task_deltas(jax.random.fold_in(key_list[3], 71), 0),
        "rank_scores": plant(jax.random.randint(key_list[1], (TASKS, LAYERS, EXPERTS * ROWS, FF), 0, 1073741824), jax.random.fold_in(key_list[1], 1), 0, 1073741823).astype(jnp.int32),
        "keep_limits": plant(jax.random.randint(key_list[2], (TASKS, LAYERS, EXPERTS), 268435456, 805306368), jax.random.fold_in(key_list[2], 1), 268435456, 805306367).astype(jnp.int32),
    }


def keep_probability(column_sums, grand_sums, row_total):
    column_mean = column_sums / row_total
    grand_mean = grand_sums / (EXPERTS * row_total * FF)
    return (0.2 + 0.7 * column_mean / (column_mean + grand_mean)).astype(jnp.bfloat16)


def reference(task_deltas, rank_scores, keep_limits):
    outputs = []
    for layer_at in range(LAYERS):
        change = task_deltas[:, layer_at].astype(jnp.float32).reshape(TASKS, EXPERTS, ROWS, FF)
        column_sums = jnp.sum(jnp.abs(change), axis=2)
        grand_sums = jnp.sum(column_sums, axis=(1, 2))
        rounded = lax.optimization_barrier(keep_probability(column_sums, grand_sums[:, None, None], ROWS))
        probability = rounded.astype(jnp.float32)
        scores = rank_scores[:, layer_at].reshape(TASKS, EXPERTS, ROWS, FF)
        limits = keep_limits[:, layer_at][:, :, None, None]
        retained = jnp.where(scores < limits, change / probability[:, :, None, :], jnp.float32(0.0))
        merged = jnp.sum(retained, axis=0).reshape(EXPERTS * ROWS, FF).astype(jnp.bfloat16)
        outputs.append(merged)
    return jnp.stack(outputs)
```

```python
import functools
import jax
import jax.numpy as jnp
from jax import lax
from jax.experimental import pallas as pl
from jax.experimental.pallas import tpu as pltpu
from jax.sharding import PartitionSpec as P

EXPERTS = 8
F32 = jnp.float32
BF16 = jnp.bfloat16
MESH = pl.DeviceIdType.MESH
BF16_MAX = float(jnp.finfo(BF16).max)
F32_MAX = float(jnp.finfo(F32).max)


def plan(layers, columns, tasks, groups):
    unit = 128 * groups
    raw = columns // 2 // unit * unit
    first = min(1024, raw // 2 // 128 * 128)
    last = min(1024, (columns - raw) // 2 // 128 * 128)
    raw_units, scaled_units = [], []
    for l in range(layers):
        for k in range(1, tasks):
            if l == 0 and k == 1:
                raw_units += [(l, k, 0, first), (l, k, first, raw - first)]
            else:
                raw_units.append((l, k, 0, raw))
            if l == layers - 1:
                cut = columns - last
                scaled_units += [(l, k, raw, cut - raw), (l, k, cut, last)]
            else:
                scaled_units.append((l, k, raw, columns - raw))
    return raw, raw_units, scaled_units


def low_size(shards):
    return 2 ** ((shards.bit_length()) // 2)


def contact_masks(shards):
    low = low_size(shards)
    return list(range(1, low)) + [low * j for j in range(1, shards // low)]


def kernel(
    sizes, delta_hbm, score_hbm, limit_hbm, merged,
    limit_ref, delta, score, outgoing, incoming, sums, sums_in, part, part_in, wide, wide_in,
    chance, chance_in, own_rate, out_rate, in_rate, own,
    limit_sem, unit_sem, rest_sem, send_sem, recv_sem, seen_sem,
    sums_sem, part_sem, wide_sem, chance_sem, share_sem,
):
    layers, rows, width, tasks, shards = sizes
    columns = width // tasks
    groups = shards // EXPERTS
    low = low_size(shards)
    all_bits = shards.bit_length() - 1
    raw, raw_units, scaled_units = plan(layers, columns, tasks, groups)
    contacts = contact_masks(shards)
    me_shard, me_task = lax.axis_index("shard"), lax.axis_index("task")
    expert = me_shard // groups
    row_total = rows * groups
    late_core = lax.rem(me_shard, 2) == 1

    def flipped(mask):
        index = me_shard
        for bit in range(all_bits):
            stride = 2**bit
            if mask & stride:
                index = index + stride * (1 - 2 * lax.rem(me_shard // stride, 2))
        return index

    def task_peer(k):
        return lax.rem(me_task + k, tasks)

    def upper(mask):
        return lax.rem(me_shard // 2 ** (mask.bit_length() - 1), 2)

    def greet(sem, mask):
        pl.semaphore_signal(sem, inc=1, device_id={"shard": flipped(mask)}, device_id_type=MESH)

    def sweep(start, length, body):
        step = length
        while step > 2048:
            step //= 2
        if step % 128:
            step = 128

        def turn(i, carry):
            body(pl.ds(pl.multiple_of(start + i * step, 128), step))
            return carry

        if length == step:
            body(pl.ds(start, length))
        else:
            lax.fori_loop(0, length // step, turn, 0)

    barrier = pltpu.get_barrier_semaphore()
    for k in range(1, tasks):
        pl.semaphore_signal(barrier, inc=1, device_id={"task": task_peer(k)}, device_id_type=MESH)

    limit_copy = pltpu.make_async_copy(limit_hbm.at[0], limit_ref, limit_sem)
    limit_copy.start()
    unit_loads = []
    for u, (l, k, c, n) in enumerate(raw_units):
        there = pl.ds(pl.multiple_of(task_peer(k) * columns + c, 128), n)
        unit_loads.append([
            pltpu.make_async_copy(whole.at[0, l, :, there], held.at[k, l, :, pl.ds(c, n)], unit_sem.at[u, j])
            for j, (whole, held) in enumerate(((score_hbm, score), (delta_hbm, delta)))
        ])
        for copy in unit_loads[u]:
            copy.start()
    rest_loads = {}
    for j, (whole, held) in enumerate(((delta_hbm, delta), (score_hbm, score))):
        for k in list(range(1, tasks)) + [0]:
            c = raw if k else 0
            there = pl.ds(pl.multiple_of(task_peer(k) * columns + c, 128), columns - c)
            rest_loads[j, k] = pltpu.make_async_copy(
                whole.at[0, :, :, there], held.at[k, :, :, pl.ds(c, columns - c)], rest_sem.at[j, k]
            )
            rest_loads[j, k].start()

    for mask in contacts:
        @pl.when(upper(mask) == 0)
        def _(mask=mask):
            greet(barrier, mask)

    def masked(l, k, at):
        limit = limit_ref[l, expert]
        return jnp.where(score[k, l, :, at] < limit, delta[k, l, :, at].astype(F32), 0.0)

    sends = []
    for u, (l, k, c, n) in enumerate(raw_units + scaled_units):
        sends.append(pltpu.make_async_remote_copy(
            src_ref=outgoing.at[k - 1, l, :, pl.ds(c, n)],
            dst_ref=incoming.at[k - 1, l, :, pl.ds(c, n)],
            send_sem=send_sem.at[u], recv_sem=recv_sem.at[u],
            device_id={"task": task_peer(k)}, device_id_type=MESH,
        ))

    limit_copy.wait()
    early = 2
    for u, (l, k, c, n) in enumerate(raw_units):
        for copy in unit_loads[u]:
            copy.wait()

        def prepare(at, l=l, k=k):
            outgoing[k - 1, l, :, at] = masked(l, k, at).astype(BF16)

        sweep(c, n, prepare)
        if u == 0:
            pl.semaphore_wait(barrier, tasks - 1 + sum(upper(mask) for mask in contacts))
        if u < early:
            sends[u].start()
        else:
            @pl.when(jnp.logical_not(late_core))
            def _(u=u):
                sends[u].start()
        if u == 0:
            for j, mask in enumerate(contacts):
                @pl.when(upper(mask) == 1)
                def _(j=j, mask=mask):
                    greet(seen_sem.at[j], mask)

    total = jnp.zeros((layers, 128), F32)
    for k in range(tasks):
        rest_loads[0, k].wait()
        for l in range(layers):

            def add_up(at, l=l, k=k):
                size = jnp.abs(delta[k, l, :, at].astype(F32))
                sums[k, l : l + 1, at] = jnp.sum(size, axis=0, keepdims=True)

            sweep(0, columns, add_up)
    step = min(2048, columns)
    for k in range(tasks):

        def gather(i, carry, k=k):
            block = sums[k, :, pl.ds(pl.multiple_of(i * step, 128), step)]
            for j in range(step // 128):
                carry = carry + block[:, j * 128 : (j + 1) * 128]
            return carry

        total = lax.fori_loop(0, columns // step, gather, total)
    part[...] = total

    for j, mask in enumerate(contacts):
        @pl.when(upper(mask) == 0)
        def _(j=j):
            pl.semaphore_wait(seen_sem.at[j], 1)

    def exchange(src, dst, sems, mask):
        copy = pltpu.make_async_remote_copy(
            src_ref=src, dst_ref=dst, send_sem=sems.at[0], recv_sem=sems.at[1],
            device_id={"shard": flipped(mask)}, device_id_type=MESH,
        )
        copy.start()
        return copy

    near = [exchange(part, part_in.at[m - 1], part_sem.at[m - 1], m) for m in range(1, low)]
    pairs = [exchange(sums, sums_in.at[m - 1], sums_sem.at[m - 1], m) for m in range(1, groups)]

    for u in range(early, len(raw_units)):
        @pl.when(late_core)
        def _(u=u):
            sends[u].start()

    for m, copy in enumerate(near):
        copy.wait()
        total = total + part_in[m]
    wide[...] = total
    far = [
        exchange(wide, wide_in.at[j - 1], wide_sem.at[j - 1], low * j) for j in range(1, shards // low)
    ]
    for copy in pairs:
        copy.wait()
    for k in range(tasks):

        def join(at, k=k):
            value = sums[k, :, at]
            for m in range(groups - 1):
                value = value + sums_in[m, k, :, at]
            sums[k, :, at] = value

        sweep(0, columns, join)
    for j, copy in enumerate(far):
        copy.wait()
        total = total + wide_in[j]
    grand_mean = jnp.sum(total, axis=1, keepdims=True) / (EXPERTS * row_total * width)

    def keep(k, at):
        mean = sums[k, :, at] / row_total
        return (0.2 + 0.7 * mean / (mean + grand_mean)).astype(BF16)

    segment = raw // groups
    mine = pl.ds(pl.multiple_of(lax.rem(me_shard, groups) * segment, 128), segment)
    chances = []
    for k in range(1, tasks):

        def fill(at, k=k):
            chance[k - 1, :, at] = keep(k, at)

        sweep(0, raw, fill)

        def invert_out(at, k=k):
            out_rate[k - 1, :, at] = 1.0 / keep(k, at).astype(F32)

        sweep(raw, columns - raw, invert_out)
        copy = pltpu.make_async_remote_copy(
            src_ref=chance.at[k - 1, :, mine], dst_ref=chance_in.at[k - 1, :, mine],
            send_sem=chance_sem.at[k - 1, 0], recv_sem=chance_sem.at[k - 1, 1],
            device_id={"task": task_peer(k)}, device_id_type=MESH,
        )
        copy.start()
        chances.append(copy)

    for k in range(1, tasks):
        rest_loads[1, k].wait()
    for u, (l, k, c, n) in enumerate(scaled_units):

        def rescale(at, l=l, k=k):
            value = masked(l, k, at) * out_rate[k - 1, l : l + 1, at]
            held = jnp.clip(value, -BF16_MAX, BF16_MAX)
            outgoing[k - 1, l, :, at] = jnp.where(jnp.abs(value) <= F32_MAX, held, value).astype(BF16)

        sweep(c, n, rescale)
        sends[len(raw_units) + u].start()

    rest_loads[1, 0].wait()

    def invert_own(at):
        own_rate[:, at] = 1.0 / keep(0, at).astype(F32)

    sweep(0, columns, invert_own)
    for l in range(layers):

        def hold(at, l=l):
            own[l, :, at] = masked(l, 0, at) * own_rate[l : l + 1, at]

        sweep(0, columns, hold)

    shares = []
    for k in range(1, tasks):
        chances[k - 1].wait()
        for mask in range(1, groups):
            shares.append(exchange(
                chance_in.at[k - 1, :, mine], chance_in.at[k - 1, :, mine], share_sem.at[k - 1, mask - 1], mask
            ))
    for copy in shares:
        copy.wait()
    for k in range(1, tasks):

        def invert_in(at, k=k):
            in_rate[k - 1, :, at] = 1.0 / chance_in[k - 1, :, at].astype(F32)

        sweep(0, raw, invert_in)

    for u, (l, k, c, n) in enumerate(raw_units):
        sends[u].wait()

        def add_raw(at, l=l, k=k):
            own[l, :, at] = own[l, :, at] + incoming[k - 1, l, :, at].astype(F32) * in_rate[k - 1, l : l + 1, at]

        if k < tasks - 1:
            sweep(c, n, add_raw)
            continue

        def end_raw(at, l=l, k=k):
            value = own[l, :, at] + incoming[k - 1, l, :, at].astype(F32) * in_rate[k - 1, l : l + 1, at]
            merged[l, :, at] = value.astype(BF16)

        sweep(c, n, end_raw)

    for u, (l, k, c, n) in enumerate(scaled_units):
        sends[len(raw_units) + u].wait()

        def add_scaled(at, l=l, k=k):
            own[l, :, at] = own[l, :, at] + incoming[k - 1, l, :, at].astype(F32)

        def end_scaled(at, l=l, k=k):
            merged[l, :, at] = (own[l, :, at] + incoming[k - 1, l, :, at].astype(F32)).astype(BF16)

        sweep(c, n, add_scaled if k < tasks - 1 else end_scaled)


def put_out(value, out_hbm, sem):
    copy = pltpu.make_async_copy(value, out_hbm, sem)
    copy.start()
    copy.wait()


def on_device(task_deltas, rank_scores, keep_limits):
    tasks, shards = lax.axis_size("task"), lax.axis_size("shard")
    _, layers, rows, width = task_deltas.shape
    columns = width // tasks
    others = max(tasks - 1, 1)
    groups = shards // EXPERTS
    low = low_size(shards)
    raw, raw_units, scaled_units = plan(layers, columns, tasks, groups)
    sent = len(raw_units) + len(scaled_units)
    dma = pltpu.SemaphoreType.DMA
    keep_limits = pltpu.with_memory_space_constraint(keep_limits, pltpu.HBM)
    result = pl.pallas_call(
        functools.partial(kernel, (layers, rows, width, tasks, shards)),
        out_shape=jax.ShapeDtypeStruct((layers, rows, columns), BF16),
        in_specs=[
            pl.BlockSpec(memory_space=pltpu.HBM),
            pl.BlockSpec(memory_space=pltpu.HBM),
            pl.BlockSpec(memory_space=pltpu.HBM),
        ],
        out_specs=pl.BlockSpec(memory_space=pltpu.VMEM),
        scratch_shapes=[
            pltpu.SMEM(keep_limits.shape[1:], jnp.int32),
            pltpu.VMEM((tasks, layers, rows, columns), BF16),
            pltpu.VMEM((tasks, layers, rows, columns), jnp.int32),
            pltpu.VMEM((others, layers, rows, columns), BF16),
            pltpu.VMEM((others, layers, rows, columns), BF16),
            pltpu.VMEM((tasks, layers, columns), F32),
            pltpu.VMEM((max(groups - 1, 1), tasks, layers, columns), F32),
            pltpu.VMEM((layers, 128), F32),
            pltpu.VMEM((max(low - 1, 1), layers, 128), F32),
            pltpu.VMEM((layers, 128), F32),
            pltpu.VMEM((max(shards // low - 1, 1), layers, 128), F32),
            pltpu.VMEM((others, layers, raw), BF16),
            pltpu.VMEM((others, layers, raw), BF16),
            pltpu.VMEM((layers, columns), F32),
            pltpu.VMEM((others, layers, columns), F32),
            pltpu.VMEM((others, layers, raw), F32),
            pltpu.VMEM((layers, rows, columns), F32),
            dma(()),
            dma((len(raw_units), 2)),
            dma((2, tasks)),
            dma((sent,)),
            dma((sent,)),
            pltpu.SemaphoreType.REGULAR((len(contact_masks(shards)),)),
            dma((max(groups - 1, 1), 2)),
            dma((max(low - 1, 1), 2)),
            dma((max(shards // low - 1, 1), 2)),
            dma((others, 2)),
            dma((others, max(groups - 1, 1), 2)),
        ],
        compiler_params=pltpu.CompilerParams(
            collective_id=0, has_side_effects=True, vmem_limit_bytes=52 * 2**20
        ),
        name="merge",
    )(task_deltas, rank_scores, keep_limits)
    return pl.pallas_call(
        put_out,
        out_shape=jax.ShapeDtypeStruct(result.shape, result.dtype),
        in_specs=[pl.BlockSpec(memory_space=pltpu.VMEM)],
        out_specs=pl.BlockSpec(memory_space=pltpu.HBM),
        scratch_shapes=[dma(())],
        compiler_params=pltpu.CompilerParams(vmem_limit_bytes=4 * 2**20),
        name="put",
    )(result)


def solution(mesh):
    return jax.shard_map(
        on_device,
        mesh=mesh,
        in_specs=(
            P("task", None, "shard", None),
            P("task", None, "shard", None),
            P("task", None, None),
        ),
        out_specs=P(None, "shard", "task"),
        check_vma=False,
    )
```

```python
import functools
import jax
import jax.numpy as jnp
from jax import lax
from jax.experimental import pallas as pl
from jax.experimental.pallas import tpu as pltpu
from jax.sharding import PartitionSpec as P

EXPERTS = 8
F32 = jnp.float32
BF16 = jnp.bfloat16
MESH = pl.DeviceIdType.MESH
BF16_MAX = float(jnp.finfo(BF16).max)
F32_MAX = float(jnp.finfo(F32).max)


HUB = 1


def plan(layers, columns, tasks, groups):
    unit = 128 * groups
    raw = columns // 2 // unit * unit
    first = min(1024, raw // 4 // 128 * 128)
    last = min(1024, (columns - raw) // 2 // 128 * 128)
    raw_units, scaled_units = [], []
    for l in range(layers):
        for k in range(1, tasks):
            if l == 0 and k == 1:
                raw_units += [(l, k, 0, first), (l, k, first, first), (l, k, 2 * first, raw - 2 * first)]
            else:
                raw_units.append((l, k, 0, raw))
            if l == layers - 1:
                cut = columns - last
                scaled_units += [(l, k, raw, cut - raw), (l, k, cut, last)]
            else:
                scaled_units.append((l, k, raw, columns - raw))
    return raw, raw_units, scaled_units


def kernel(
    sizes, delta_hbm, score_hbm, limit_hbm, merged,
    limit_ref, delta, score, outgoing, incoming, sums, sums_in, part, part_in, total_ref,
    chance, chance_in, own_rate, out_rate, in_rate, own,
    limit_sem, unit_sem, later_sem, rest_sem, send_sem, recv_sem,
    sums_sem, part_send, part_recv, total_send, total_recv, chance_sem, share_sem,
):
    layers, rows, width, tasks, shards = sizes
    columns = width // tasks
    groups = shards // EXPERTS
    all_bits = shards.bit_length() - 1
    raw, raw_units, scaled_units = plan(layers, columns, tasks, groups)
    me_shard, me_task = lax.axis_index("shard"), lax.axis_index("task")
    expert = me_shard // groups
    row_total = rows * groups
    late_core = lax.rem(me_shard, 2) == 1
    is_hub = me_shard == HUB
    outside = [s for s in range(shards) if s // groups != HUB // groups]

    def flipped(mask):
        index = me_shard
        for bit in range(all_bits):
            stride = 2**bit
            if mask & stride:
                index = index + stride * (1 - 2 * lax.rem(me_shard // stride, 2))
        return index

    def task_peer(k):
        return lax.rem(me_task + k, tasks)

    def sweep(start, length, body):
        step = length
        while step > 2048:
            step //= 2
        if step % 128:
            step = 128

        def turn(i, carry):
            body(pl.ds(pl.multiple_of(start + i * step, 128), step))
            return carry

        if length == step:
            body(pl.ds(start, length))
        else:
            lax.fori_loop(0, length // step, turn, 0)

    barrier = pltpu.get_barrier_semaphore()
    for k in range(1, tasks):
        pl.semaphore_signal(barrier, inc=1, device_id={"task": task_peer(k)}, device_id_type=MESH)
    for mask in range(1, groups):
        pl.semaphore_signal(barrier, inc=1, device_id={"shard": flipped(mask)}, device_id_type=MESH)

    limit_copy = pltpu.make_async_copy(limit_hbm.at[0], limit_ref, limit_sem)
    limit_copy.start()

    def load(whole, held, k, ls, c, n, sem):
        there = pl.ds(pl.multiple_of(task_peer(k) * columns + c, 128), n)
        copy = pltpu.make_async_copy(whole.at[0, ls, :, there], held.at[k, ls, :, pl.ds(c, n)], sem)
        copy.start()
        return copy

    every, later = pl.ds(0, layers), pl.ds(1, layers - 1)
    unit_loads = {}
    for u, (l, k, c, n) in enumerate(raw_units):
        if l == 0:
            unit_loads[u] = [
                load(score_hbm, score, k, l, c, n, unit_sem.at[u, 0]),
                load(delta_hbm, delta, k, l, c, n, unit_sem.at[u, 1]),
            ]
    later_loads = {k: load(delta_hbm, delta, k, later, 0, columns, later_sem.at[k]) for k in range(1, tasks)}
    for u, (l, k, c, n) in enumerate(raw_units):
        if l:
            unit_loads[u] = [load(score_hbm, score, k, l, c, n, unit_sem.at[u, 0])]
    delta_loads = [
        load(delta_hbm, delta, k, 0, raw, columns - raw, rest_sem.at[0, k]) if k
        else load(delta_hbm, delta, 0, every, 0, columns, rest_sem.at[0, 0])
        for k in list(range(1, tasks)) + [0]
    ]
    score_loads = {
        k: load(score_hbm, score, k, every, raw if k else 0, columns - (raw if k else 0), rest_sem.at[1, k])
        for k in list(range(1, tasks)) + [0]
    }

    @pl.when(is_hub)
    def _():
        for s in outside:
            pl.semaphore_signal(barrier, inc=1, device_id={"shard": s}, device_id_type=MESH)

    def masked(l, k, at):
        limit = limit_ref[l, expert]
        return jnp.where(score[k, l, :, at] < limit, delta[k, l, :, at].astype(F32), 0.0)

    sends = []
    for u, (l, k, c, n) in enumerate(raw_units + scaled_units):
        sends.append(pltpu.make_async_remote_copy(
            src_ref=outgoing.at[k - 1, l, :, pl.ds(c, n)],
            dst_ref=incoming.at[k - 1, l, :, pl.ds(c, n)],
            send_sem=send_sem.at[u], recv_sem=recv_sem.at[u],
            device_id={"task": task_peer(k)}, device_id_type=MESH,
        ))

    limit_copy.wait()
    early = 2
    for u, (l, k, c, n) in enumerate(raw_units):
        if l and later_loads:
            for copy in later_loads.values():
                copy.wait()
            later_loads = None
        for copy in unit_loads[u]:
            copy.wait()

        def prepare(at, l=l, k=k):
            outgoing[k - 1, l, :, at] = masked(l, k, at).astype(BF16)

        sweep(c, n, prepare)
        if u == 0:
            away = jnp.where(expert == HUB // groups, 0, 1)
            pl.semaphore_wait(barrier, tasks - 1 + groups - 1 + away)
        if u < early:
            sends[u].start()
        else:
            @pl.when(jnp.logical_not(late_core))
            def _(u=u):
                sends[u].start()

    total = jnp.zeros((layers, 128), F32)
    for copy in delta_loads:
        copy.wait()
    for k in range(tasks):
        for l in range(layers):

            def add_up(at, l=l, k=k):
                size = jnp.abs(delta[k, l, :, at].astype(F32))
                sums[k, l : l + 1, at] = jnp.sum(size, axis=0, keepdims=True)

            sweep(0, columns, add_up)
    step = min(2048, columns)
    for k in range(tasks):

        def gather(i, carry, k=k):
            block = sums[k, :, pl.ds(pl.multiple_of(i * step, 128), step)]
            for j in range(step // 128):
                carry = carry + block[:, j * 128 : (j + 1) * 128]
            return carry

        total = lax.fori_loop(0, columns // step, gather, total)
    part[...] = total

    def exchange(src, dst, sems, mask):
        copy = pltpu.make_async_remote_copy(
            src_ref=src, dst_ref=dst, send_sem=sems.at[0], recv_sem=sems.at[1],
            device_id={"shard": flipped(mask)}, device_id_type=MESH,
        )
        copy.start()
        return copy

    pairs = [exchange(sums, sums_in.at[m - 1], sums_sem.at[m - 1], m) for m in range(1, groups)]

    def to_shard(src, dst, send, recv, s):
        return pltpu.make_async_remote_copy(
            src_ref=src, dst_ref=dst, send_sem=send, recv_sem=recv, device_id={"shard": s}, device_id_type=MESH
        )

    others = [s for s in range(shards) if s != HUB]
    to_hub = to_shard(part, part_in.at[me_shard], part_send, part_recv.at[me_shard], HUB)
    to_all = {s: to_shard(total_ref, total_ref, total_send.at[s], total_recv, s) for s in others}

    @pl.when(jnp.logical_not(is_hub))
    def _():
        to_hub.start()

    for u in range(early, len(raw_units)):
        @pl.when(late_core)
        def _(u=u):
            sends[u].start()

    for copy in pairs:
        copy.wait()
    for k in range(tasks):

        def join(at, k=k):
            value = sums[k, :, at]
            for m in range(groups - 1):
                value = value + sums_in[m, k, :, at]
            sums[k, :, at] = value

        sweep(0, columns, join)
    @pl.when(is_hub)
    def _():
        value = part[...]
        for s in others:
            to_shard(part, part_in.at[s], part_send, part_recv.at[s], s).wait_recv()
            value = value + part_in[s]
        total_ref[...] = value
        for s in others:
            to_all[s].start()

    @pl.when(jnp.logical_not(is_hub))
    def _():
        to_all[others[0]].wait_recv()
        to_hub.wait_send()

    total = total_ref[...]
    grand_mean = jnp.sum(total, axis=1, keepdims=True) / (EXPERTS * row_total * width)

    def keep(k, at):
        mean = sums[k, :, at] / row_total
        return (0.2 + 0.7 * mean / (mean + grand_mean)).astype(BF16)

    segment = raw // groups
    mine = pl.ds(pl.multiple_of(lax.rem(me_shard, groups) * segment, 128), segment)
    chances = []
    for k in range(1, tasks):

        def fill(at, k=k):
            chance[k - 1, :, at] = keep(k, at)

        sweep(0, raw, fill)

        def invert_out(at, k=k):
            out_rate[k - 1, :, at] = 1.0 / keep(k, at).astype(F32)

        sweep(raw, columns - raw, invert_out)
        copy = pltpu.make_async_remote_copy(
            src_ref=chance.at[k - 1, :, mine], dst_ref=chance_in.at[k - 1, :, mine],
            send_sem=chance_sem.at[k - 1, 0], recv_sem=chance_sem.at[k - 1, 1],
            device_id={"task": task_peer(k)}, device_id_type=MESH,
        )
        copy.start()
        chances.append(copy)

    for k in range(1, tasks):
        score_loads[k].wait()
    for u, (l, k, c, n) in enumerate(scaled_units):

        def rescale(at, l=l, k=k):
            value = masked(l, k, at) * out_rate[k - 1, l : l + 1, at]
            held = jnp.clip(value, -BF16_MAX, BF16_MAX)
            outgoing[k - 1, l, :, at] = jnp.where(jnp.abs(value) <= F32_MAX, held, value).astype(BF16)

        sweep(c, n, rescale)
        sends[len(raw_units) + u].start()

    score_loads[0].wait()

    def invert_own(at):
        own_rate[:, at] = 1.0 / keep(0, at).astype(F32)

    sweep(0, columns, invert_own)
    for l in range(layers):

        def hold(at, l=l):
            own[l, :, at] = masked(l, 0, at) * own_rate[l : l + 1, at]

        sweep(0, columns, hold)

    shares = []
    for k in range(1, tasks):
        chances[k - 1].wait()
        for mask in range(1, groups):
            shares.append(exchange(
                chance_in.at[k - 1, :, mine], chance_in.at[k - 1, :, mine], share_sem.at[k - 1, mask - 1], mask
            ))
    for copy in shares:
        copy.wait()
    for k in range(1, tasks):

        def invert_in(at, k=k):
            in_rate[k - 1, :, at] = 1.0 / chance_in[k - 1, :, at].astype(F32)

        sweep(0, raw, invert_in)

    for u, (l, k, c, n) in enumerate(raw_units):
        sends[u].wait()

        def add_raw(at, l=l, k=k):
            own[l, :, at] = own[l, :, at] + incoming[k - 1, l, :, at].astype(F32) * in_rate[k - 1, l : l + 1, at]

        if k < tasks - 1:
            sweep(c, n, add_raw)
            continue

        def end_raw(at, l=l, k=k):
            value = own[l, :, at] + incoming[k - 1, l, :, at].astype(F32) * in_rate[k - 1, l : l + 1, at]
            merged[l, :, at] = value.astype(BF16)

        sweep(c, n, end_raw)

    @pl.when(is_hub)
    def _():
        for s in others:
            to_all[s].wait_send()

    for u, (l, k, c, n) in enumerate(scaled_units):
        sends[len(raw_units) + u].wait()

        def add_scaled(at, l=l, k=k):
            own[l, :, at] = own[l, :, at] + incoming[k - 1, l, :, at].astype(F32)

        def end_scaled(at, l=l, k=k):
            merged[l, :, at] = (own[l, :, at] + incoming[k - 1, l, :, at].astype(F32)).astype(BF16)

        sweep(c, n, add_scaled if k < tasks - 1 else end_scaled)


def put_out(value, out_hbm, sem):
    copy = pltpu.make_async_copy(value, out_hbm, sem)
    copy.start()
    copy.wait()


def on_device(task_deltas, rank_scores, keep_limits):
    tasks, shards = lax.axis_size("task"), lax.axis_size("shard")
    _, layers, rows, width = task_deltas.shape
    columns = width // tasks
    others = max(tasks - 1, 1)
    groups = shards // EXPERTS
    raw, raw_units, scaled_units = plan(layers, columns, tasks, groups)
    sent = len(raw_units) + len(scaled_units)
    dma = pltpu.SemaphoreType.DMA
    keep_limits = pltpu.with_memory_space_constraint(keep_limits, pltpu.HBM)
    result = pl.pallas_call(
        functools.partial(kernel, (layers, rows, width, tasks, shards)),
        out_shape=jax.ShapeDtypeStruct((layers, rows, columns), BF16),
        in_specs=[
            pl.BlockSpec(memory_space=pltpu.HBM),
            pl.BlockSpec(memory_space=pltpu.HBM),
            pl.BlockSpec(memory_space=pltpu.HBM),
        ],
        out_specs=pl.BlockSpec(memory_space=pltpu.VMEM),
        scratch_shapes=[
            pltpu.SMEM(keep_limits.shape[1:], jnp.int32),
            pltpu.VMEM((tasks, layers, rows, columns), BF16),
            pltpu.VMEM((tasks, layers, rows, columns), jnp.int32),
            pltpu.VMEM((others, layers, rows, columns), BF16),
            pltpu.VMEM((others, layers, rows, columns), BF16),
            pltpu.VMEM((tasks, layers, columns), F32),
            pltpu.VMEM((max(groups - 1, 1), tasks, layers, columns), F32),
            pltpu.VMEM((layers, 128), F32),
            pltpu.VMEM((shards, layers, 128), F32),
            pltpu.VMEM((layers, 128), F32),
            pltpu.VMEM((others, layers, raw), BF16),
            pltpu.VMEM((others, layers, raw), BF16),
            pltpu.VMEM((layers, columns), F32),
            pltpu.VMEM((others, layers, columns), F32),
            pltpu.VMEM((others, layers, raw), F32),
            pltpu.VMEM((layers, rows, columns), F32),
            dma(()),
            dma((len(raw_units), 2)),
            dma((tasks,)),
            dma((2, tasks)),
            dma((sent,)),
            dma((sent,)),
            dma((max(groups - 1, 1), 2)),
            dma(()),
            dma((shards,)),
            dma((shards,)),
            dma(()),
            dma((others, 2)),
            dma((others, max(groups - 1, 1), 2)),
        ],
        compiler_params=pltpu.CompilerParams(
            collective_id=0, has_side_effects=True, vmem_limit_bytes=52 * 2**20
        ),
        name="merge",
    )(task_deltas, rank_scores, keep_limits)
    return pl.pallas_call(
        put_out,
        out_shape=jax.ShapeDtypeStruct(result.shape, result.dtype),
        in_specs=[pl.BlockSpec(memory_space=pltpu.VMEM)],
        out_specs=pl.BlockSpec(memory_space=pltpu.HBM),
        scratch_shapes=[dma(())],
        compiler_params=pltpu.CompilerParams(vmem_limit_bytes=4 * 2**20),
        name="put",
    )(result)


def solution(mesh):
    return jax.shard_map(
        on_device,
        mesh=mesh,
        in_specs=(
            P("task", None, "shard", None),
            P("task", None, "shard", None),
            P("task", None, None),
        ),
        out_specs=P(None, "shard", "task"),
        check_vma=False,
    )
```

```python
import functools
import jax
import jax.numpy as jnp
from jax import lax
from jax.experimental import pallas as pl
from jax.experimental.pallas import tpu as pltpu
from jax.sharding import PartitionSpec as P

EXPERTS = 8
F32 = jnp.float32
BF16 = jnp.bfloat16
MESH = pl.DeviceIdType.MESH
BF16_MAX = float(jnp.finfo(BF16).max)
F32_MAX = float(jnp.finfo(F32).max)


HUB = 1


def plan(layers, columns, tasks, groups):
    unit = 128 * groups
    raw = columns // 2 // unit * unit
    first = min(1024, raw // 4 // 128 * 128)
    last = min(1024, (columns - raw) // 4 // 128 * 128)
    raw_units, scaled_units = [], []
    for k in range(1, tasks):
        if k == 1:
            raw_units += [(k, 0, 1, 0, first), (k, 0, 1, first, first), (k, 0, 1, 2 * first, raw - 2 * first)]
        else:
            raw_units.append((k, 0, 1, 0, raw))
    for k in range(1, tasks):
        raw_units.append((k, 1, layers - 1, 0, raw))
    for k in range(1, tasks):
        scaled_units += [(k, 0, 1, raw, columns - raw), (k, 1, layers - 2, raw, columns - raw)]
    for k in range(1, tasks):
        cut = columns - last
        scaled_units += [(k, layers - 1, 1, raw, cut - raw), (k, layers - 1, 1, cut, last)]
    return raw, raw_units, scaled_units


def detours(columns, tasks, shards, groups):
    if tasks != 2:
        return [], 0
    return [HUB + groups * j for j in range(1, 4) if HUB + groups * j < shards], columns // 16 // 128 * 128


def kernel(
    sizes, delta_hbm, score_hbm, limit_hbm, merged,
    limit_ref, delta, score, outgoing, incoming, sums, sums_in, part, part_in, total_ref,
    chance, chance_in, own_rate, out_rate, in_rate, own, detoured,
    limit_sem, unit_sem, rest_sem, send_sem, recv_sem,
    sums_sem, part_send, part_recv, total_send, total_recv, chance_sem, share_sem, leg_sem,
):
    layers, rows, width, tasks, shards = sizes
    columns = width // tasks
    groups = shards // EXPERTS
    all_bits = shards.bit_length() - 1
    raw, raw_units, scaled_units = plan(layers, columns, tasks, groups)
    me_shard, me_task = lax.axis_index("shard"), lax.axis_index("task")
    expert = me_shard // groups
    row_total = rows * groups
    late_core = lax.rem(me_shard, 2) == 1
    is_hub = me_shard == HUB
    outside = [s for s in range(shards) if s // groups != HUB // groups]

    def flipped(mask):
        index = me_shard
        for bit in range(all_bits):
            stride = 2**bit
            if mask & stride:
                index = index + stride * (1 - 2 * lax.rem(me_shard // stride, 2))
        return index

    def task_peer(k):
        return lax.rem(me_task + k, tasks)

    def sweep(start, length, body):
        step = length
        while step > 2048:
            step //= 2
        if step % 128:
            step = 128

        def turn(i, carry):
            body(pl.ds(pl.multiple_of(start + i * step, 128), step))
            return carry

        if length == step:
            body(pl.ds(start, length))
        else:
            lax.fori_loop(0, length // step, turn, 0)

    barrier = pltpu.get_barrier_semaphore()
    for k in range(1, tasks):
        pl.semaphore_signal(barrier, inc=1, device_id={"task": task_peer(k)}, device_id_type=MESH)
    for mask in range(1, groups):
        pl.semaphore_signal(barrier, inc=1, device_id={"shard": flipped(mask)}, device_id_type=MESH)

    limit_copy = pltpu.make_async_copy(limit_hbm.at[0], limit_ref, limit_sem)
    limit_copy.start()

    def load(whole, held, k, ls, c, n, sem):
        there = pl.ds(pl.multiple_of(task_peer(k) * columns + c, 128), n)
        copy = pltpu.make_async_copy(whole.at[0, ls, :, there], held.at[k, ls, :, pl.ds(c, n)], sem)
        copy.start()
        return copy

    unit_loads = []
    for u, (k, l, deep, c, n) in enumerate(raw_units):
        wide = 0 if l == 0 else columns - n
        unit_loads.append([
            load(score_hbm, score, k, pl.ds(l, deep), c, n, unit_sem.at[u, 0]),
            load(delta_hbm, delta, k, pl.ds(l, deep), c, n + wide, unit_sem.at[u, 1]),
        ])
    every = pl.ds(0, layers)
    ks = list(range(1, tasks)) + [0]
    delta_loads = [
        load(delta_hbm, delta, k, pl.ds(0, 1) if k else every, raw if k else 0, columns - (raw if k else 0), rest_sem.at[0, k])
        for k in ks
    ]
    score_loads = {
        k: load(score_hbm, score, k, every, raw if k else 0, columns - (raw if k else 0), rest_sem.at[1, k])
        for k in ks
    }

    @pl.when(is_hub)
    def _():
        for s in outside:
            pl.semaphore_signal(barrier, inc=1, device_id={"shard": s}, device_id_type=MESH)

    def masked(l, k, at):
        limit = limit_ref[l, expert]
        return jnp.where(score[k, l, :, at] < limit, delta[k, l, :, at].astype(F32), 0.0)

    def to_task(u, k, l, deep, c, n):
        where = (k - 1, pl.ds(l, deep), slice(None), pl.ds(c, n))
        return pltpu.make_async_remote_copy(
            src_ref=outgoing.at[where], dst_ref=incoming.at[where],
            send_sem=send_sem.at[u], recv_sem=recv_sem.at[u],
            device_id={"task": task_peer(k)}, device_id_type=MESH,
        )

    def to_shard(src, dst, send, recv, s, task=None):
        where = {"shard": s} if task is None else {"shard": s, "task": task}
        return pltpu.make_async_remote_copy(
            src_ref=src, dst_ref=dst, send_sem=send, recv_sem=recv, device_id=where, device_id_type=MESH
        )

    sends = [to_task(u, *unit) for u, unit in enumerate(raw_units + scaled_units)]
    split = len(raw_units) + len(scaled_units) - 2
    helpers, detour = detours(columns, tasks, shards, groups)
    hub_sends = jnp.logical_and(is_hub, me_task == 1)
    hub_takes = jnp.logical_and(is_hub, me_task == 0)
    if helpers:
        k, l, deep, c, n = (raw_units + scaled_units)[split]
        skipped = detour * len(helpers)
        hub_copy = to_task(split, k, l, deep, c + skipped, n - skipped)
        legs = []
        for j, s in enumerate(helpers):
            at = pl.ds(c + j * detour, detour)
            legs.append((
                to_shard(outgoing.at[0, l, :, at], detoured.at[j], leg_sem.at[j, 0], leg_sem.at[j, 1], s, 0),
                to_shard(detoured.at[j], incoming.at[0, l, :, at], leg_sem.at[j, 2], leg_sem.at[j, 3], HUB),
            ))

    limit_copy.wait()
    early = 2
    for u, (k, l, deep, c, n) in enumerate(raw_units):
        for copy in unit_loads[u]:
            copy.wait()
        for layer in range(l, l + deep):

            def prepare(at, layer=layer, k=k):
                outgoing[k - 1, layer, :, at] = masked(layer, k, at).astype(BF16)

            sweep(c, n, prepare)
        if u == 0:
            away = jnp.where(expert == HUB // groups, 0, 1)
            pl.semaphore_wait(barrier, tasks - 1 + groups - 1 + away)
        if u < early:
            sends[u].start()
        else:
            @pl.when(jnp.logical_not(late_core))
            def _(u=u):
                sends[u].start()

    total = jnp.zeros((layers, 128), F32)
    for copy in delta_loads:
        copy.wait()
    for k in range(tasks):
        for l in range(layers):

            def add_up(at, l=l, k=k):
                size = jnp.abs(delta[k, l, :, at].astype(F32))
                sums[k, l : l + 1, at] = jnp.sum(size, axis=0, keepdims=True)

            sweep(0, columns, add_up)
    step = min(2048, columns)
    for k in range(tasks):

        def gather(i, carry, k=k):
            block = sums[k, :, pl.ds(pl.multiple_of(i * step, 128), step)]
            for j in range(step // 128):
                carry = carry + block[:, j * 128 : (j + 1) * 128]
            return carry

        total = lax.fori_loop(0, columns // step, gather, total)
    part[...] = total

    def exchange(src, dst, sems, mask):
        copy = pltpu.make_async_remote_copy(
            src_ref=src, dst_ref=dst, send_sem=sems.at[0], recv_sem=sems.at[1],
            device_id={"shard": flipped(mask)}, device_id_type=MESH,
        )
        copy.start()
        return copy

    pairs = [exchange(sums, sums_in.at[m - 1], sums_sem.at[m - 1], m) for m in range(1, groups)]

    others = [s for s in range(shards) if s != HUB]
    to_hub = to_shard(part, part_in.at[me_shard], part_send, part_recv.at[me_shard], HUB)
    to_all = {s: to_shard(total_ref, total_ref, total_send.at[s], total_recv, s) for s in others}

    @pl.when(jnp.logical_not(is_hub))
    def _():
        to_hub.start()

    for copy in pairs:
        copy.wait()
    for u in range(early, len(raw_units)):
        @pl.when(late_core)
        def _(u=u):
            sends[u].start()

    for k in range(tasks):

        def join(at, k=k):
            value = sums[k, :, at]
            for m in range(groups - 1):
                value = value + sums_in[m, k, :, at]
            sums[k, :, at] = value

        sweep(0, columns, join)
    @pl.when(is_hub)
    def _():
        value = part[...]
        for s in others:
            to_shard(part, part_in.at[s], part_send, part_recv.at[s], s).wait_recv()
            value = value + part_in[s]
        total_ref[...] = value
        for s in others:
            to_all[s].start()

    @pl.when(jnp.logical_not(is_hub))
    def _():
        to_all[others[0]].wait_recv()
        to_hub.wait_send()

    total = total_ref[...]
    grand_mean = jnp.sum(total, axis=1, keepdims=True) / (EXPERTS * row_total * width)

    def keep(k, at):
        mean = sums[k, :, at] / row_total
        return (0.2 + 0.7 * mean / (mean + grand_mean)).astype(BF16)

    segment = raw // groups
    mine = pl.ds(pl.multiple_of(lax.rem(me_shard, groups) * segment, 128), segment)
    chances = []
    for k in range(1, tasks):

        def fill(at, k=k):
            chance[k - 1, :, at] = keep(k, at)

        sweep(0, raw, fill)

        def invert_out(at, k=k):
            out_rate[k - 1, :, at] = 1.0 / keep(k, at).astype(F32)

        sweep(raw, columns - raw, invert_out)
        copy = pltpu.make_async_remote_copy(
            src_ref=chance.at[k - 1, :, mine], dst_ref=chance_in.at[k - 1, :, mine],
            send_sem=chance_sem.at[k - 1, 0], recv_sem=chance_sem.at[k - 1, 1],
            device_id={"task": task_peer(k)}, device_id_type=MESH,
        )
        copy.start()
        chances.append(copy)

    for k in range(1, tasks):
        score_loads[k].wait()
    for u, (k, l, deep, c, n) in enumerate(scaled_units, len(raw_units)):
        for layer in range(l, l + deep):

            def rescale(at, layer=layer, k=k):
                value = masked(layer, k, at) * out_rate[k - 1, layer : layer + 1, at]
                held = jnp.clip(value, -BF16_MAX, BF16_MAX)
                outgoing[k - 1, layer, :, at] = jnp.where(jnp.abs(value) <= F32_MAX, held, value).astype(BF16)

            sweep(c, n, rescale)
        if helpers and u == split:
            @pl.when(hub_sends)
            def _():
                for there, _ in legs:
                    there.start()
                hub_copy.start()

            @pl.when(jnp.logical_not(hub_sends))
            def _():
                sends[split].start()
        else:
            sends[u].start()

    score_loads[0].wait()

    def invert_own(at):
        own_rate[:, at] = 1.0 / keep(0, at).astype(F32)

    sweep(0, columns, invert_own)
    for l in range(layers):

        def hold(at, l=l):
            own[l, :, at] = masked(l, 0, at) * own_rate[l : l + 1, at]

        sweep(0, columns, hold)

    shares = []
    for k in range(1, tasks):
        chances[k - 1].wait()
        for mask in range(1, groups):
            shares.append(exchange(
                chance_in.at[k - 1, :, mine], chance_in.at[k - 1, :, mine], share_sem.at[k - 1, mask - 1], mask
            ))
    for copy in shares:
        copy.wait()
    for k in range(1, tasks):

        def invert_in(at, k=k):
            in_rate[k - 1, :, at] = 1.0 / chance_in[k - 1, :, at].astype(F32)

        sweep(0, raw, invert_in)

    def combine(k, l, deep, c, n, scaled):
        for layer in range(l, l + deep):

            def add(at, layer=layer):
                value = incoming[k - 1, layer, :, at].astype(F32)
                if not scaled:
                    value = value * in_rate[k - 1, layer : layer + 1, at]
                value = own[layer, :, at] + value
                if k < tasks - 1:
                    own[layer, :, at] = value
                else:
                    merged[layer, :, at] = value.astype(BF16)

            sweep(c, n, add)

    for u, unit in enumerate(raw_units):
        sends[u].wait()
        combine(*unit, scaled=False)

    for j, s in enumerate(helpers):
        @pl.when(jnp.logical_and(me_shard == s, me_task == 0))
        def _(j=j):
            legs[j][0].wait_recv()
            legs[j][1].start()

    @pl.when(is_hub)
    def _():
        for s in others:
            to_all[s].wait_send()

    for u, unit in enumerate(scaled_units, len(raw_units)):
        if helpers and u == split:
            @pl.when(hub_takes)
            def _():
                for _, on in legs:
                    on.wait_recv()
                hub_copy.wait_recv()
                sends[split].wait_send()

            @pl.when(hub_sends)
            def _():
                for there, _ in legs:
                    there.wait_send()
                hub_copy.wait_send()
                sends[split].wait_recv()

            @pl.when(jnp.logical_not(is_hub))
            def _():
                sends[split].wait()

            for j, s in enumerate(helpers):
                @pl.when(jnp.logical_and(me_shard == s, me_task == 0))
                def _(j=j):
                    legs[j][1].wait_send()
        else:
            sends[u].wait()
        combine(*unit, scaled=True)


def put_out(value, out_hbm, sem):
    copy = pltpu.make_async_copy(value, out_hbm, sem)
    copy.start()
    copy.wait()


def on_device(task_deltas, rank_scores, keep_limits):
    tasks, shards = lax.axis_size("task"), lax.axis_size("shard")
    _, layers, rows, width = task_deltas.shape
    columns = width // tasks
    others = max(tasks - 1, 1)
    groups = shards // EXPERTS
    raw, raw_units, scaled_units = plan(layers, columns, tasks, groups)
    helpers, detour = detours(columns, tasks, shards, groups)
    pieces = max(len(helpers), 1)
    sent = len(raw_units) + len(scaled_units)
    dma = pltpu.SemaphoreType.DMA
    keep_limits = pltpu.with_memory_space_constraint(keep_limits, pltpu.HBM)
    result = pl.pallas_call(
        functools.partial(kernel, (layers, rows, width, tasks, shards)),
        out_shape=jax.ShapeDtypeStruct((layers, rows, columns), BF16),
        in_specs=[
            pl.BlockSpec(memory_space=pltpu.HBM),
            pl.BlockSpec(memory_space=pltpu.HBM),
            pl.BlockSpec(memory_space=pltpu.HBM),
        ],
        out_specs=pl.BlockSpec(memory_space=pltpu.VMEM),
        scratch_shapes=[
            pltpu.SMEM(keep_limits.shape[1:], jnp.int32),
            pltpu.VMEM((tasks, layers, rows, columns), BF16),
            pltpu.VMEM((tasks, layers, rows, columns), jnp.int32),
            pltpu.VMEM((others, layers, rows, columns), BF16),
            pltpu.VMEM((others, layers, rows, columns), BF16),
            pltpu.VMEM((tasks, layers, columns), F32),
            pltpu.VMEM((max(groups - 1, 1), tasks, layers, columns), F32),
            pltpu.VMEM((layers, 128), F32),
            pltpu.VMEM((shards, layers, 128), F32),
            pltpu.VMEM((layers, 128), F32),
            pltpu.VMEM((others, layers, raw), BF16),
            pltpu.VMEM((others, layers, raw), BF16),
            pltpu.VMEM((layers, columns), F32),
            pltpu.VMEM((others, layers, columns), F32),
            pltpu.VMEM((others, layers, raw), F32),
            pltpu.VMEM((layers, rows, columns), F32),
            pltpu.VMEM((pieces, rows, max(detour, 128)), BF16),
            dma(()),
            dma((len(raw_units), 2)),
            dma((2, tasks)),
            dma((sent,)),
            dma((sent,)),
            dma((max(groups - 1, 1), 2)),
            dma(()),
            dma((shards,)),
            dma((shards,)),
            dma(()),
            dma((others, 2)),
            dma((others, max(groups - 1, 1), 2)),
            dma((pieces, 4)),
        ],
        compiler_params=pltpu.CompilerParams(
            collective_id=0, has_side_effects=True, vmem_limit_bytes=52 * 2**20
        ),
        name="merge",
    )(task_deltas, rank_scores, keep_limits)
    return pl.pallas_call(
        put_out,
        out_shape=jax.ShapeDtypeStruct(result.shape, result.dtype),
        in_specs=[pl.BlockSpec(memory_space=pltpu.VMEM)],
        out_specs=pl.BlockSpec(memory_space=pltpu.HBM),
        scratch_shapes=[dma(())],
        compiler_params=pltpu.CompilerParams(vmem_limit_bytes=4 * 2**20),
        name="put",
    )(result)


def solution(mesh):
    return jax.shard_map(
        on_device,
        mesh=mesh,
        in_specs=(
            P("task", None, "shard", None),
            P("task", None, "shard", None),
            P("task", None, None),
        ),
        out_specs=P(None, "shard", "task"),
        check_vma=False,
    )
```

```python
import functools
import jax
import jax.numpy as jnp
from jax import lax
from jax.experimental import pallas as pl
from jax.experimental.pallas import tpu as pltpu
from jax.sharding import PartitionSpec as P

EXPERTS = 8
F32 = jnp.float32
BF16 = jnp.bfloat16
MESH = pl.DeviceIdType.MESH
BF16_MAX = float(jnp.finfo(BF16).max)
F32_MAX = float(jnp.finfo(F32).max)
HUB = 1


def plan(layers, columns, tasks, groups):
    unit = 128 * groups
    raw = columns // 2 // unit * unit
    first = min(512, raw // 4 // 128 * 128)
    last = min(1024, (columns - raw) // 4 // 128 * 128)
    cut = columns - last
    ks = range(1, tasks)
    raw_units = [(1, 0, 1, 0, first), (1, 0, 1, first, first), (1, 0, 1, 2 * first, raw - 2 * first)]
    raw_units += [(k, 0, 1, 0, raw) for k in ks if k > 1]
    raw_units += [(k, 1, layers - 1, 0, raw) for k in ks]
    scaled_units = [(k, 0, 1, raw, columns - raw) for k in ks]
    scaled_units += [(k, 1, layers - 2, raw, columns - raw) for k in ks]
    scaled_units += [(k, layers - 1, 1, raw, cut - raw) for k in ks]
    scaled_units += [(k, layers - 1, 1, cut, last) for k in ks]
    return raw, first, cut, raw_units, scaled_units


def detours(columns, tasks, shards, groups):
    if tasks != 2:
        return [], 0
    return [HUB + groups * j for j in range(1, 4) if HUB + groups * j < shards], columns * 5 // 64 // 128 * 128


def kernel(
    sizes, delta_hbm, score_hbm, limit_hbm, merged,
    limit_ref, delta, score, outgoing, incoming, sums, sums_in, part, part_in, total_ref,
    chance, chance_in, own_rate, out_rate, in_rate, own, detoured,
    load_sem, send_sem, recv_sem, sums_sem, hub_sem, chance_sem, leg_sem,
):
    layers, rows, width, tasks, shards = sizes
    columns = width // tasks
    groups = shards // EXPERTS
    all_bits = shards.bit_length() - 1
    raw, first, cut, raw_units, scaled_units = plan(layers, columns, tasks, groups)
    ks = list(range(1, tasks))
    me_shard, me_task = lax.axis_index("shard"), lax.axis_index("task")
    expert = me_shard // groups
    row_total = rows * groups
    is_hub = me_shard == HUB
    not_hub = jnp.logical_not(is_hub)
    others = [s for s in range(shards) if s != HUB]
    outside = [s for s in others if s // groups != HUB // groups]
    helpers, detour = detours(columns, tasks, shards, groups)

    def flipped(mask):
        index = me_shard
        for bit in range(all_bits):
            stride = 2**bit
            if mask & stride:
                index = index + stride * (1 - 2 * lax.rem(me_shard // stride, 2))
        return index

    def task_peer(k):
        return lax.rem(me_task + k, tasks)

    def remote(src, dst, send, recv, where):
        return pltpu.make_async_remote_copy(
            src_ref=src, dst_ref=dst, send_sem=send, recv_sem=recv, device_id=where, device_id_type=MESH
        )

    def sweep(start, length, body):
        step = length
        while step > 2048:
            step //= 2
        if step % 128:
            step = 128

        def turn(i, carry):
            body(pl.ds(pl.multiple_of(start + i * step, 128), step))
            return carry

        if length == step:
            body(pl.ds(start, length))
        else:
            lax.fori_loop(0, length // step, turn, 0)

    barrier = pltpu.get_barrier_semaphore()

    def greet(where):
        pl.semaphore_signal(barrier, inc=1, device_id=where, device_id_type=MESH)

    used = []

    def load(whole, held, k, l, deep, c, n):
        there = pl.ds(pl.multiple_of(task_peer(k) * columns + c, 128), n)
        copy = pltpu.make_async_copy(
            whole.at[0, pl.ds(l, deep), :, there], held.at[k, pl.ds(l, deep), :, pl.ds(c, n)],
            load_sem.at[len(used)],
        )
        used.append(copy)
        copy.start()
        return copy

    limit_copy = pltpu.make_async_copy(limit_hbm.at[0], limit_ref, load_sem.at[0])
    used.append(limit_copy)
    limit_copy.start()
    first_loads = [load(score_hbm, score, 1, 0, 1, 0, first), load(delta_hbm, delta, 1, 0, 1, 0, first)]
    for k in ks:
        greet({"task": task_peer(k)})
    for mask in range(1, groups):
        greet({"shard": flipped(mask)})
    top_loads, deep_loads, own_loads = [], [], []
    for k in ks:
        c = first if k == 1 else 0
        top_loads.append(load(score_hbm, score, k, 0, 1, c, raw - c))
        top_loads.append(load(delta_hbm, delta, k, 0, 1, c, columns - c))
    for k in ks:
        deep_loads.append(load(score_hbm, score, k, 1, layers - 1, 0, raw))
        deep_loads.append(load(delta_hbm, delta, k, 1, layers - 1, 0, columns))
    own_loads.append(load(delta_hbm, delta, 0, 0, layers, 0, columns))
    score_loads = [load(score_hbm, score, k, 0, layers, raw, columns - raw) for k in ks]
    own_score_load = load(score_hbm, score, 0, 0, layers, 0, columns)

    @pl.when(is_hub)
    def _():
        for s in outside:
            greet({"shard": s})

    def masked(l, k, at):
        limit = limit_ref[l, expert]
        return jnp.where(score[k, l, :, at] < limit, delta[k, l, :, at].astype(F32), 0.0)

    def to_task(k, l, deep, c, n, recv):
        where = (k - 1, pl.ds(l, deep), slice(None), pl.ds(c, n))
        return remote(outgoing.at[where], incoming.at[where], send_sem, recv_sem.at[recv], {"task": task_peer(k)})

    raw_sends = [to_task(*unit, 0) for unit in raw_units]
    scaled_sends = [to_task(*unit, 1 + u // (2 * len(ks)) + u // (3 * len(ks))) for u, unit in enumerate(scaled_units)]
    hub_sends = jnp.logical_and(is_hub, me_task == 1)
    split = len(scaled_units) - 2
    legs = []
    if helpers:
        k, l, deep, c, n = scaled_units[split]
        skipped = detour * len(helpers)
        hub_copy = to_task(k, l, deep, c + skipped, n - skipped, 2)
        for j, s in enumerate(helpers):
            at = pl.ds(c + j * detour, detour)
            legs.append((
                remote(outgoing.at[0, l, :, at], detoured, send_sem, leg_sem.at[0], {"shard": s, "task": 0}),
                remote(detoured, incoming.at[0, l, :, at], leg_sem.at[1], recv_sem.at[2], {"shard": HUB}),
            ))

    limit_copy.wait()
    early = 3
    held_back = jnp.logical_and(is_hub, tasks > 1)
    for u, (k, l, deep, c, n) in enumerate(raw_units):
        if u == 0:
            ready = first_loads
        elif u == 1:
            ready = top_loads
        elif l:
            ready, deep_loads = deep_loads, []
            own_loads = own_loads
        for copy in ready:
            copy.wait()
        ready = []
        for layer in range(l, l + deep):

            def prepare(at, layer=layer, k=k):
                outgoing[k - 1, layer, :, at] = masked(layer, k, at).astype(BF16)

            sweep(c, n, prepare)
        if u == 0:
            away = jnp.where(expert == HUB // groups, 0, 1)
            pl.semaphore_wait(barrier, tasks - 1 + groups - 1 + away)
        if u < early:
            raw_sends[u].start()
        else:
            @pl.when(jnp.logical_not(held_back))
            def _(u=u):
                raw_sends[u].start()

    for copy in own_loads:
        copy.wait()
    for k in range(tasks):
        for l in range(layers):

            def add_up(at, l=l, k=k):
                size = jnp.abs(delta[k, l, :, at].astype(F32))
                sums[k, l : l + 1, at] = jnp.sum(size, axis=0, keepdims=True)

            sweep(0, columns, add_up)
    total = jnp.zeros((layers, 128), F32)
    step = min(2048, columns)
    for k in range(tasks):

        def gather(i, carry, k=k):
            block = sums[k, :, pl.ds(pl.multiple_of(i * step, 128), step)]
            for j in range(step // 128):
                carry = carry + block[:, j * 128 : (j + 1) * 128]
            return carry

        total = lax.fori_loop(0, columns // step, gather, total)
    part[...] = total

    slot = lax.rem(me_shard + (shards - 1 - HUB), shards)
    to_hub = remote(part, part_in.at[slot], hub_sem.at[0], hub_sem.at[1], {"shard": HUB})
    to_all = [remote(total_ref, total_ref, hub_sem.at[0], hub_sem.at[1], {"shard": s}) for s in others]
    all_parts = remote(
        part_in.at[pl.ds(0, shards - 1)], part_in.at[pl.ds(0, shards - 1)], hub_sem.at[0], hub_sem.at[1], {"shard": HUB}
    )

    @pl.when(not_hub)
    def _():
        to_hub.start()

    for m in range(1, groups):
        remote(sums, sums_in.at[m - 1], sums_sem.at[0], sums_sem.at[1], {"shard": flipped(m)}).start()
    if groups > 1:
        pair_wait = remote(sums_in, sums_in, sums_sem.at[0], sums_sem.at[1], {"shard": HUB})
        pair_wait.wait_send()
        pair_wait.wait_recv()

    for u in range(early, len(raw_units)):
        @pl.when(held_back)
        def _(u=u):
            raw_sends[u].start()

    for k in range(tasks):

        def join(at, k=k):
            value = sums[k, :, at]
            for m in range(groups - 1):
                value = value + sums_in[m, k, :, at]
            sums[k, :, at] = value

        sweep(0, columns, join)

    @pl.when(is_hub)
    def _():
        all_parts.wait_recv()
        value = part[...]
        for s in range(shards - 1):
            value = value + part_in[s]
        total_ref[...] = value
        for copy in to_all:
            copy.start()

    @pl.when(not_hub)
    def _():
        to_all[0].wait_recv()

    total = total_ref[...]
    grand_mean = jnp.sum(total, axis=1, keepdims=True) / (EXPERTS * row_total * width)

    def keep(k, at):
        mean = sums[k, :, at] / row_total
        return (0.2 + 0.7 * mean / (mean + grand_mean)).astype(BF16)

    segment = raw // groups
    mine = pl.ds(pl.multiple_of(lax.rem(me_shard, groups) * segment, 128), segment)
    for k in ks:

        def fill(at, k=k):
            chance[k - 1, :, at] = keep(k, at)

        sweep(0, raw, fill)

        def invert_out(at, k=k):
            out_rate[k - 1, :, at] = 1.0 / keep(k, at).astype(F32)

        sweep(raw, columns - raw, invert_out)
        remote(
            chance.at[k - 1, :, mine], chance_in.at[k - 1, :, mine], chance_sem.at[0], chance_sem.at[1],
            {"task": task_peer(k)},
        ).start()

    for copy in score_loads:
        copy.wait()
    for u, (k, l, deep, c, n) in enumerate(scaled_units):
        for layer in range(l, l + deep):

            def rescale(at, layer=layer, k=k):
                value = masked(layer, k, at) * out_rate[k - 1, layer : layer + 1, at]
                held = jnp.clip(value, -BF16_MAX, BF16_MAX)
                outgoing[k - 1, layer, :, at] = jnp.where(jnp.abs(value) <= F32_MAX, held, value).astype(BF16)

            sweep(c, n, rescale)
        if helpers and u == split:
            @pl.when(hub_sends)
            def _():
                for there, _ in legs:
                    there.start()
                hub_copy.start()

            @pl.when(jnp.logical_not(hub_sends))
            def _():
                scaled_sends[split].start()
        else:
            scaled_sends[u].start()

    own_score_load.wait()

    def invert_own(at):
        own_rate[:, at] = 1.0 / keep(0, at).astype(F32)

    sweep(0, columns, invert_own)
    for l in range(layers):

        def hold(at, l=l):
            own[l, :, at] = masked(l, 0, at) * own_rate[l : l + 1, at]

        sweep(0, columns, hold)

    if ks:
        got = chance_in.at[:, :, mine]
        remote(got, got, chance_sem.at[0], chance_sem.at[1], {"shard": HUB}).wait_recv()
        for k in ks:
            for mask in range(1, groups):
                piece = chance_in.at[k - 1, :, mine]
                remote(piece, piece, chance_sem.at[0], chance_sem.at[2], {"shard": flipped(mask)}).start()
        if groups > 1:
            shared = chance_in.at[:, :, pl.ds(0, segment * (groups - 1))]
            remote(shared, shared, chance_sem.at[0], chance_sem.at[2], {"shard": HUB}).wait_recv()
    for k in ks:

        def invert_in(at, k=k):
            in_rate[k - 1, :, at] = 1.0 / chance_in[k - 1, :, at].astype(F32)

        sweep(0, raw, invert_in)

    def arrived(recv, l, deep, c, n):
        piece = incoming.at[:, pl.ds(l, deep), :, pl.ds(c, n)]
        remote(piece, piece, send_sem, recv_sem.at[recv], {"shard": HUB}).wait_recv()

    def combine(l, deep, c, n, scaled):
        for layer in range(l, l + deep):

            def add(at, layer=layer):
                total = own[layer, :, at]
                for k in ks:
                    value = incoming[k - 1, layer, :, at].astype(F32)
                    if not scaled:
                        value = value * in_rate[k - 1, layer : layer + 1, at]
                    total = total + value
                merged[layer, :, at] = total.astype(BF16)

            sweep(c, n, add)

    arrived(0, 0, layers, 0, raw)
    combine(0, layers, 0, raw, False)

    for j, s in enumerate(helpers):
        @pl.when(jnp.logical_and(me_shard == s, me_task == 0))
        def _(j=j):
            legs[j][0].wait_recv()
            legs[j][1].start()

    arrived(1, 0, layers - 1, raw, columns - raw)
    combine(0, layers - 1, raw, columns - raw, True)
    arrived(2, layers - 1, 1, raw, cut - raw)
    combine(layers - 1, 1, raw, cut - raw, True)
    remote(chance_in, chance_in, chance_sem.at[0], chance_sem.at[1], {"shard": HUB}).wait_send()

    @pl.when(is_hub)
    def _():
        all_parts.wait_send()

    @pl.when(not_hub)
    def _():
        to_hub.wait_send()

    for j, s in enumerate(helpers):
        @pl.when(jnp.logical_and(me_shard == s, me_task == 0))
        def _(j=j):
            legs[j][1].wait_send()

    arrived(3, layers - 1, 1, cut, columns - cut)
    combine(layers - 1, 1, cut, columns - cut, True)
    remote(outgoing, outgoing, send_sem, recv_sem.at[0], {"shard": HUB}).wait_send()


def put_out(value, out_hbm, sem):
    copy = pltpu.make_async_copy(value, out_hbm, sem)
    copy.start()
    copy.wait()


def on_device(task_deltas, rank_scores, keep_limits):
    tasks, shards = lax.axis_size("task"), lax.axis_size("shard")
    _, layers, rows, width = task_deltas.shape
    columns = width // tasks
    others = tasks - 1
    groups = shards // EXPERTS
    raw, _, _, _, _ = plan(layers, columns, tasks, groups)
    _, detour = detours(columns, tasks, shards, groups)
    dma = pltpu.SemaphoreType.DMA
    keep_limits = pltpu.with_memory_space_constraint(keep_limits, pltpu.HBM)
    result = pl.pallas_call(
        functools.partial(kernel, (layers, rows, width, tasks, shards)),
        out_shape=jax.ShapeDtypeStruct((layers, rows, columns), BF16),
        in_specs=[
            pl.BlockSpec(memory_space=pltpu.HBM),
            pl.BlockSpec(memory_space=pltpu.HBM),
            pl.BlockSpec(memory_space=pltpu.HBM),
        ],
        out_specs=pl.BlockSpec(memory_space=pltpu.VMEM),
        scratch_shapes=[
            pltpu.SMEM(keep_limits.shape[1:], jnp.int32),
            pltpu.VMEM((tasks, layers, rows, columns), BF16),
            pltpu.VMEM((tasks, layers, rows, columns), jnp.int32),
            pltpu.VMEM((others, layers, rows, columns), BF16),
            pltpu.VMEM((others, layers, rows, columns), BF16),
            pltpu.VMEM((tasks, layers, columns), F32),
            pltpu.VMEM((max(groups - 1, 1), tasks, layers, columns), F32),
            pltpu.VMEM((layers, 128), F32),
            pltpu.VMEM((shards - 1, layers, 128), F32),
            pltpu.VMEM((layers, 128), F32),
            pltpu.VMEM((others, layers, raw), BF16),
            pltpu.VMEM((others, layers, raw), BF16),
            pltpu.VMEM((layers, columns), F32),
            pltpu.VMEM((others, layers, columns), F32),
            pltpu.VMEM((others, layers, raw), F32),
            pltpu.VMEM((layers, rows, columns), F32),
            pltpu.VMEM((rows, max(detour, 128)), BF16),
            dma((3 + 5 * others + 2,)),
            dma(()),
            dma((4,)),
            dma((2,)),
            dma((2,)),
            dma((3,)),
            dma((2,)),
        ],
        compiler_params=pltpu.CompilerParams(
            collective_id=0, has_side_effects=True, vmem_limit_bytes=52 * 2**20
        ),
        name="merge",
    )(task_deltas, rank_scores, keep_limits)
    return pl.pallas_call(
        put_out,
        out_shape=jax.ShapeDtypeStruct(result.shape, result.dtype),
        in_specs=[pl.BlockSpec(memory_space=pltpu.VMEM)],
        out_specs=pl.BlockSpec(memory_space=pltpu.HBM),
        scratch_shapes=[dma(())],
        compiler_params=pltpu.CompilerParams(vmem_limit_bytes=4 * 2**20),
        name="put",
    )(result)


def solution(mesh):
    return jax.shard_map(
        on_device,
        mesh=mesh,
        in_specs=(
            P("task", None, "shard", None),
            P("task", None, "shard", None),
            P("task", None, None),
        ),
        out_specs=P(None, "shard", "task"),
        check_vma=False,
    )
```

```python
import functools
import jax
import jax.numpy as jnp
from jax import lax
from jax.experimental import pallas as pl
from jax.experimental.pallas import tpu as pltpu
from jax.sharding import PartitionSpec as P

EXPERTS = 8
F32 = jnp.float32
BF16 = jnp.bfloat16
MESH = pl.DeviceIdType.MESH
BF16_MAX = float(jnp.finfo(BF16).max)
F32_MAX = float(jnp.finfo(F32).max)
HUB = 1


def plan(layers, columns, tasks, groups):
    unit = 128 * groups
    raw = columns // 2 // unit * unit
    first = min(512, raw // 4 // 128 * 128)
    last = min(1024, (columns - raw) // 4 // 128 * 128)
    cut = columns - last
    ks = range(1, tasks)
    raw_units = [(1, 0, 1, 0, first), (1, 0, 1, first, first), (1, 0, 1, 2 * first, raw - 2 * first)]
    raw_units += [(k, 0, 1, 0, raw) for k in ks if k > 1]
    raw_units += [(k, 1, layers - 1, 0, raw) for k in ks]
    scaled_units = [(k, 0, 1, raw, columns - raw) for k in ks]
    scaled_units += [(k, 1, layers - 2, raw, columns - raw) for k in ks]
    scaled_units += [(k, layers - 1, 1, raw, cut - raw) for k in ks]
    scaled_units += [(k, layers - 1, 1, cut, last) for k in ks]
    return raw, first, cut, raw_units, scaled_units


def detours(columns, tasks, shards, groups):
    if tasks != 2:
        return [], 0
    return [HUB + groups * j for j in range(1, 4) if HUB + groups * j < shards], columns * 5 // 64 // 128 * 128


def kernel(
    sizes, delta_hbm, score_hbm, limit_hbm, merged,
    limit_ref, delta, score, outgoing, incoming, sums, sums_in, part, part_in, total_ref,
    chance, chance_in, own_rate, out_rate, in_rate, own, detoured,
    load_sem, send_sem, recv_sem, sums_sem, hub_sem, chance_sem, leg_sem,
):
    layers, rows, width, tasks, shards = sizes
    columns = width // tasks
    groups = shards // EXPERTS
    all_bits = shards.bit_length() - 1
    raw, first, cut, raw_units, scaled_units = plan(layers, columns, tasks, groups)
    ks = list(range(1, tasks))
    me_shard, me_task = lax.axis_index("shard"), lax.axis_index("task")
    expert = me_shard // groups
    row_total = rows * groups
    is_hub = me_shard == HUB
    not_hub = jnp.logical_not(is_hub)
    others = [s for s in range(shards) if s != HUB]
    outside = [s for s in others if s // groups != HUB // groups]
    helpers, detour = detours(columns, tasks, shards, groups)

    def flipped(mask):
        index = me_shard
        for bit in range(all_bits):
            stride = 2**bit
            if mask & stride:
                index = index + stride * (1 - 2 * lax.rem(me_shard // stride, 2))
        return index

    def task_peer(k):
        return lax.rem(me_task + k, tasks)

    def remote(src, dst, send, recv, where):
        return pltpu.make_async_remote_copy(
            src_ref=src, dst_ref=dst, send_sem=send, recv_sem=recv, device_id=where, device_id_type=MESH
        )

    def sweep(start, length, body):
        step = length
        while step > 2048:
            step //= 2
        if step % 128:
            step = 128

        def turn(i, carry):
            body(pl.ds(pl.multiple_of(start + i * step, 128), step))
            return carry

        if length == step:
            body(pl.ds(start, length))
        else:
            lax.fori_loop(0, length // step, turn, 0)

    barrier = pltpu.get_barrier_semaphore()

    def greet(where):
        pl.semaphore_signal(barrier, inc=1, device_id=where, device_id_type=MESH)

    used = []

    def load(whole, held, k, l, deep, c, n, again=None):
        there = pl.ds(pl.multiple_of(task_peer(k) * columns + c, 128), n)
        copy = pltpu.make_async_copy(
            whole.at[0, pl.ds(l, deep), :, there], held.at[k, pl.ds(l, deep), :, pl.ds(c, n)],
            load_sem.at[len(used) if again is None else again],
        )
        if again is None:
            used.append(copy)
        copy.start()
        return copy

    limit_copy = pltpu.make_async_copy(limit_hbm.at[0], limit_ref, load_sem.at[0])
    used.append(limit_copy)
    limit_copy.start()
    first_loads = [load(score_hbm, score, 1, 0, 1, 0, first), load(delta_hbm, delta, 1, 0, 1, 0, first)]
    for k in ks:
        greet({"task": task_peer(k)})
    for mask in range(1, groups):
        greet({"shard": flipped(mask)})
    top_loads, deep_loads, own_loads = [], [], []
    second_loads = [load(score_hbm, score, 1, 0, 1, first, first), load(delta_hbm, delta, 1, 0, 1, first, first)]
    for k in ks:
        c = 2 * first if k == 1 else 0
        top_loads.append(load(score_hbm, score, k, 0, 1, c, raw - c))
        top_loads.append(load(delta_hbm, delta, k, 0, 1, c, raw - c))
    for k in ks:
        deep_loads.append(load(score_hbm, score, k, 1, layers - 1, 0, raw))
        deep_loads.append(load(delta_hbm, delta, k, 1, layers - 1, 0, columns))
    own_loads += [load(delta_hbm, delta, k, 0, 1, raw, columns - raw) for k in ks]
    own_loads.append(load(delta_hbm, delta, 0, 0, layers, 0, columns))

    @pl.when(is_hub)
    def _():
        for s in outside:
            greet({"shard": s})

    def masked(l, k, at):
        limit = limit_ref[l, expert]
        return jnp.where(score[k, l, :, at] < limit, delta[k, l, :, at].astype(F32), 0.0)

    def to_task(k, l, deep, c, n, recv):
        where = (k - 1, pl.ds(l, deep), slice(None), pl.ds(c, n))
        return remote(outgoing.at[where], incoming.at[where], send_sem, recv_sem.at[recv], {"task": task_peer(k)})

    raw_sends = [to_task(*unit, 0) for unit in raw_units]
    scaled_sends = [to_task(*unit, 1 + u // (2 * len(ks)) + u // (3 * len(ks))) for u, unit in enumerate(scaled_units)]
    hub_sends = jnp.logical_and(is_hub, me_task == 1)
    split = len(scaled_units) - 2
    legs = []
    if helpers:
        k, l, deep, c, n = scaled_units[split]
        skipped = detour * len(helpers)
        hub_copy = to_task(k, l, deep, c + skipped, n - skipped, 2)
        for j, s in enumerate(helpers):
            at = pl.ds(c + j * detour, detour)
            legs.append((
                remote(outgoing.at[0, l, :, at], detoured, send_sem, leg_sem, {"shard": s, "task": 0}),
                remote(detoured, incoming.at[0, l, :, at], load_sem.at[1], recv_sem.at[2], {"shard": HUB}),
            ))

    limit_copy.wait()
    early = 3
    held_back = jnp.logical_and(is_hub, tasks > 1)
    slow = jnp.logical_and(lax.rem(me_shard, 2) == 1, not_hub)
    for u, (k, l, deep, c, n) in enumerate(raw_units):
        if u == 0:
            ready = first_loads
        elif u == 1:
            ready = second_loads
        elif u == 2:
            ready = top_loads
        elif l:
            ready, deep_loads = deep_loads, []
            own_loads = own_loads
        for copy in ready:
            copy.wait()
        ready = []
        for layer in range(l, l + deep):

            def prepare(at, layer=layer, k=k):
                outgoing[k - 1, layer, :, at] = masked(layer, k, at).astype(BF16)

            sweep(c, n, prepare)
        if u == 0:
            away = jnp.where(expert == HUB // groups, 0, 1)
            pl.semaphore_wait(barrier, tasks - 1 + groups - 1 + away)
        if u < 3:
            raw_sends[u].start()
        elif u < early:
            @pl.when(jnp.logical_not(slow))
            def _(u=u):
                raw_sends[u].start()
        else:
            @pl.when(lax.rem(me_shard, 2) == 0)
            def _(u=u):
                raw_sends[u].start()

    score_loads = [load(score_hbm, score, k, 0, layers, raw, columns - raw, 2 + k) for k in ks]
    own_score_load = load(score_hbm, score, 0, 0, layers, 0, columns, 1)
    for copy in own_loads:
        copy.wait()
    for k in range(tasks):
        for l in range(layers):

            def add_up(at, l=l, k=k):
                size = jnp.abs(delta[k, l, :, at].astype(F32))
                sums[k, l : l + 1, at] = jnp.sum(size, axis=0, keepdims=True)

            sweep(0, columns, add_up)
    total = jnp.zeros((layers, 128), F32)
    step = min(2048, columns)
    for k in range(tasks):

        def gather(i, carry, k=k):
            block = sums[k, :, pl.ds(pl.multiple_of(i * step, 128), step)]
            for j in range(step // 128):
                carry = carry + block[:, j * 128 : (j + 1) * 128]
            return carry

        total = lax.fori_loop(0, columns // step, gather, total)
    part[...] = total
    for u in range(3, len(raw_units)):
        @pl.when(slow)
        def _(u=u):
            raw_sends[u].start()


    slot = lax.rem(me_shard + (shards - 1 - HUB), shards)
    to_hub = remote(part, part_in.at[slot], load_sem.at[2], hub_sem, {"shard": HUB})
    to_all = [remote(total_ref, total_ref, load_sem.at[2], hub_sem, {"shard": s}) for s in others]
    all_parts = remote(
        part_in.at[pl.ds(0, shards - 1)], part_in.at[pl.ds(0, shards - 1)], load_sem.at[2], hub_sem, {"shard": HUB}
    )

    @pl.when(not_hub)
    def _():
        to_hub.start()

    for m in range(1, groups):
        remote(sums, sums_in.at[m - 1], load_sem.at[0], sums_sem, {"shard": flipped(m)}).start()
    if groups > 1:
        pair_wait = remote(sums_in, sums_in, load_sem.at[0], sums_sem, {"shard": HUB})
        pair_wait.wait_send()
        pair_wait.wait_recv()

    for u in range(early, len(raw_units)):
        @pl.when(held_back)
        def _(u=u):
            raw_sends[u].start()

    for k in range(tasks):

        def join(at, k=k):
            value = sums[k, :, at]
            for m in range(groups - 1):
                value = value + sums_in[m, k, :, at]
            sums[k, :, at] = value

        sweep(0, columns, join)

    @pl.when(is_hub)
    def _():
        all_parts.wait_recv()
        value = part[...]
        for s in range(shards - 1):
            value = value + part_in[s]
        total_ref[...] = value
        for copy in to_all:
            copy.start()

    @pl.when(not_hub)
    def _():
        to_all[0].wait_recv()

    total = total_ref[...]
    grand_mean = jnp.sum(total, axis=1, keepdims=True) / (EXPERTS * row_total * width)

    def keep(k, at):
        mean = sums[k, :, at] / row_total
        return (0.2 + 0.7 * mean / (mean + grand_mean)).astype(BF16)

    segment = raw // groups
    mine = pl.ds(pl.multiple_of(lax.rem(me_shard, groups) * segment, 128), segment)
    for k in ks:

        def fill(at, k=k):
            chance[k - 1, :, at] = keep(k, at)

        sweep(0, raw, fill)

        def invert_out(at, k=k):
            out_rate[k - 1, :, at] = 1.0 / keep(k, at).astype(F32)

        sweep(raw, columns - raw, invert_out)
        remote(
            chance.at[k - 1, :, mine], chance_in.at[k - 1, :, mine], load_sem.at[0], chance_sem.at[0],
            {"task": task_peer(k)},
        ).start()

    for copy in score_loads:
        copy.wait()
    for u, (k, l, deep, c, n) in enumerate(scaled_units):
        for layer in range(l, l + deep):

            def rescale(at, layer=layer, k=k):
                value = masked(layer, k, at) * out_rate[k - 1, layer : layer + 1, at]
                held = jnp.clip(value, -BF16_MAX, BF16_MAX)
                outgoing[k - 1, layer, :, at] = jnp.where(jnp.abs(value) <= F32_MAX, held, value).astype(BF16)

            sweep(c, n, rescale)
        if helpers and u == split:
            @pl.when(hub_sends)
            def _():
                for there, _ in legs:
                    there.start()
                hub_copy.start()

            @pl.when(jnp.logical_not(hub_sends))
            def _():
                scaled_sends[split].start()
        else:
            scaled_sends[u].start()

    own_score_load.wait()

    def invert_own(at):
        own_rate[:, at] = 1.0 / keep(0, at).astype(F32)

    sweep(0, columns, invert_own)
    for l in range(layers):

        def hold(at, l=l):
            own[l, :, at] = masked(l, 0, at) * own_rate[l : l + 1, at]

        sweep(0, columns, hold)

    if ks:
        got = chance_in.at[:, :, mine]
        remote(got, got, load_sem.at[0], chance_sem.at[0], {"shard": HUB}).wait_recv()
        for k in ks:
            for mask in range(1, groups):
                piece = chance_in.at[k - 1, :, mine]
                remote(piece, piece, load_sem.at[0], chance_sem.at[1], {"shard": flipped(mask)}).start()
        if groups > 1:
            shared = chance_in.at[:, :, pl.ds(0, segment * (groups - 1))]
            remote(shared, shared, load_sem.at[0], chance_sem.at[1], {"shard": HUB}).wait_recv()
    for k in ks:

        def invert_in(at, k=k):
            in_rate[k - 1, :, at] = 1.0 / chance_in[k - 1, :, at].astype(F32)

        sweep(0, raw, invert_in)

    def arrived(recv, l, deep, c, n):
        piece = incoming.at[:, pl.ds(l, deep), :, pl.ds(c, n)]
        remote(piece, piece, send_sem, recv_sem.at[recv], {"shard": HUB}).wait_recv()

    def combine(l, deep, c, n, scaled):
        for layer in range(l, l + deep):

            def add(at, layer=layer):
                total = own[layer, :, at]
                for k in ks:
                    value = incoming[k - 1, layer, :, at].astype(F32)
                    if not scaled:
                        value = value * in_rate[k - 1, layer : layer + 1, at]
                    total = total + value
                merged[layer, :, at] = total.astype(BF16)

            sweep(c, n, add)

    arrived(0, 0, layers, 0, raw)
    combine(0, layers, 0, raw, False)

    for j, s in enumerate(helpers):
        @pl.when(jnp.logical_and(me_shard == s, me_task == 0))
        def _(j=j):
            legs[j][0].wait_recv()
            legs[j][1].start()

    arrived(1, 0, layers - 1, raw, columns - raw)
    combine(0, layers - 1, raw, columns - raw, True)
    arrived(2, layers - 1, 1, raw, cut - raw)
    combine(layers - 1, 1, raw, cut - raw, True)
    remote(chance_in, chance_in, load_sem.at[0], chance_sem.at[0], {"shard": HUB}).wait_send()

    @pl.when(is_hub)
    def _():
        all_parts.wait_send()

    @pl.when(not_hub)
    def _():
        to_hub.wait_send()

    for j, s in enumerate(helpers):
        @pl.when(jnp.logical_and(me_shard == s, me_task == 0))
        def _(j=j):
            legs[j][1].wait_send()

    arrived(3, layers - 1, 1, cut, columns - cut)
    combine(layers - 1, 1, cut, columns - cut, True)
    remote(outgoing, outgoing, send_sem, recv_sem.at[0], {"shard": HUB}).wait_send()


def put_out(value, out_hbm, sem):
    copy = pltpu.make_async_copy(value, out_hbm, sem)
    copy.start()
    copy.wait()


def on_device(task_deltas, rank_scores, keep_limits):
    tasks, shards = lax.axis_size("task"), lax.axis_size("shard")
    _, layers, rows, width = task_deltas.shape
    columns = width // tasks
    others = tasks - 1
    groups = shards // EXPERTS
    raw, _, _, _, _ = plan(layers, columns, tasks, groups)
    _, detour = detours(columns, tasks, shards, groups)
    dma = pltpu.SemaphoreType.DMA
    keep_limits = pltpu.with_memory_space_constraint(keep_limits, pltpu.HBM)
    result = pl.pallas_call(
        functools.partial(kernel, (layers, rows, width, tasks, shards)),
        out_shape=jax.ShapeDtypeStruct((layers, rows, columns), BF16),
        in_specs=[
            pl.BlockSpec(memory_space=pltpu.HBM),
            pl.BlockSpec(memory_space=pltpu.HBM),
            pl.BlockSpec(memory_space=pltpu.HBM),
        ],
        out_specs=pl.BlockSpec(memory_space=pltpu.VMEM),
        scratch_shapes=[
            pltpu.SMEM(keep_limits.shape[1:], jnp.int32),
            pltpu.VMEM((tasks, layers, rows, columns), BF16),
            pltpu.VMEM((tasks, layers, rows, columns), jnp.int32),
            pltpu.VMEM((others, layers, rows, columns), BF16),
            pltpu.VMEM((others, layers, rows, columns), BF16),
            pltpu.VMEM((tasks, layers, columns), F32),
            pltpu.VMEM((max(groups - 1, 1), tasks, layers, columns), F32),
            pltpu.VMEM((layers, 128), F32),
            pltpu.VMEM((shards - 1, layers, 128), F32),
            pltpu.VMEM((layers, 128), F32),
            pltpu.VMEM((others, layers, raw), BF16),
            pltpu.VMEM((others, layers, raw), BF16),
            pltpu.VMEM((layers, columns), F32),
            pltpu.VMEM((others, layers, columns), F32),
            pltpu.VMEM((others, layers, raw), F32),
            pltpu.VMEM((layers, rows, columns), F32),
            pltpu.VMEM((rows, max(detour, 128)), BF16),
            dma((6 + 5 * others,)),
            dma(()),
            dma((4,)),
            dma(()),
            dma(()),
            dma((2,)),
            dma(()),
        ],
        compiler_params=pltpu.CompilerParams(
            collective_id=0, has_side_effects=True, vmem_limit_bytes=52 * 2**20
        ),
        name="merge",
    )(task_deltas, rank_scores, keep_limits)
    return pl.pallas_call(
        put_out,
        out_shape=jax.ShapeDtypeStruct(result.shape, result.dtype),
        in_specs=[pl.BlockSpec(memory_space=pltpu.VMEM)],
        out_specs=pl.BlockSpec(memory_space=pltpu.HBM),
        scratch_shapes=[dma(())],
        compiler_params=pltpu.CompilerParams(vmem_limit_bytes=4 * 2**20),
        name="put",
    )(result)


def solution(mesh):
    return jax.shard_map(
        on_device,
        mesh=mesh,
        in_specs=(
            P("task", None, "shard", None),
            P("task", None, "shard", None),
            P("task", None, None),
        ),
        out_specs=P(None, "shard", "task"),
        check_vma=False,
    )
```

```python
import functools
import jax
import jax.numpy as jnp
from jax import lax
from jax.experimental import pallas as pl
from jax.experimental.pallas import tpu as pltpu
from jax.sharding import PartitionSpec as P

EXPERTS = 8
F32 = jnp.float32
BF16 = jnp.bfloat16
MESH = pl.DeviceIdType.MESH
BF16_MAX = float(jnp.finfo(BF16).max)
F32_MAX = float(jnp.finfo(F32).max)
HUB = 1


def plan(layers, columns, tasks, groups):
    unit = 128 * groups
    raw = columns // 2 // unit * unit
    first = min(512, raw // 4 // 128 * 128)
    last = min(1024, (columns - raw) // 4 // 128 * 128)
    cut = columns - last
    ks = range(1, tasks)
    raw_units = [(1, 0, 1, 0, first), (1, 0, 1, first, first), (1, 0, 1, 2 * first, raw - 2 * first)]
    raw_units += [(k, 0, 1, 0, raw) for k in ks if k > 1]
    raw_units += [(k, 1, layers - 1, 0, raw) for k in ks]
    scaled_units = [(k, 0, 1, raw, columns - raw) for k in ks]
    scaled_units += [(k, 1, layers - 2, raw, columns - raw) for k in ks]
    scaled_units += [(k, layers - 1, 1, raw, cut - raw) for k in ks]
    scaled_units += [(k, layers - 1, 1, cut, last) for k in ks]
    return raw, first, cut, raw_units, scaled_units


def detours(layers, columns, tasks, shards, groups):
    helpers = list(range(HUB + groups, shards, groups)) if tasks == 2 else []
    if not helpers:
        return [], 0
    room = plan(layers, columns, tasks, groups)[4][-2][4]
    return helpers, min(columns * 3 // 64, room * 7 // 8 // len(helpers)) // 128 * 128


def kernel(
    sizes, delta_hbm, score_hbm, limit_hbm, merged,
    limit_ref, delta, score, outgoing, incoming, sums, sums_in, part, part_in, total_ref,
    chance, chance_in, own_rate, out_rate, in_rate, own, detoured,
    load_sem, send_sem, recv_sem, sums_sem, hub_sem, chance_sem, leg_sem,
):
    layers, rows, width, tasks, shards = sizes
    columns = width // tasks
    groups = shards // EXPERTS
    all_bits = shards.bit_length() - 1
    raw, first, cut, raw_units, scaled_units = plan(layers, columns, tasks, groups)
    ks = list(range(1, tasks))
    me_shard, me_task = lax.axis_index("shard"), lax.axis_index("task")
    expert = me_shard // groups
    row_total = rows * groups
    is_hub = me_shard == HUB
    not_hub = jnp.logical_not(is_hub)
    others = [s for s in range(shards) if s != HUB]
    outside = [s for s in others if s // groups != HUB // groups]
    helpers, detour = detours(layers, columns, tasks, shards, groups)

    def flipped(mask):
        index = me_shard
        for bit in range(all_bits):
            stride = 2**bit
            if mask & stride:
                index = index + stride * (1 - 2 * lax.rem(me_shard // stride, 2))
        return index

    def task_peer(k):
        return lax.rem(me_task + k, tasks)

    def remote(src, dst, send, recv, where):
        return pltpu.make_async_remote_copy(
            src_ref=src, dst_ref=dst, send_sem=send, recv_sem=recv, device_id=where, device_id_type=MESH
        )

    def sweep(start, length, body):
        step = length
        while step > 2048:
            step //= 2
        if step % 128:
            step = 128

        def turn(i, carry):
            body(pl.ds(pl.multiple_of(start + i * step, 128), step))
            return carry

        if length == step:
            body(pl.ds(start, length))
        else:
            lax.fori_loop(0, length // step, turn, 0)

    barrier = pltpu.get_barrier_semaphore()

    def greet(where):
        pl.semaphore_signal(barrier, inc=1, device_id=where, device_id_type=MESH)

    used = []

    def load(whole, held, k, l, deep, c, n, sem):
        there = pl.ds(pl.multiple_of(task_peer(k) * columns + c, 128), n)
        copy = pltpu.make_async_copy(
            whole.at[0, pl.ds(l, deep), :, there], held.at[k, pl.ds(l, deep), :, pl.ds(c, n)], load_sem.at[sem]
        )
        copy.start()
        return copy

    def load_both(k, l, deep, c, n, more=0):
        sem = 1 + len(used)
        load(score_hbm, score, k, l, deep, c, n, sem)
        load(delta_hbm, delta, k, l, deep, c, n + more, sem)
        both = pl.ds(0, n + (n + more) // 2)
        used.append(pltpu.make_async_copy(
            score_hbm.at[0, pl.ds(l, deep), :, both], score.at[k, pl.ds(l, deep), :, both], load_sem.at[sem]
        ))
        return used[-1]

    first_load = load_both(1, 0, 1, 0, first)
    limit_copy = pltpu.make_async_copy(limit_hbm.at[0], limit_ref, load_sem.at[0])
    limit_copy.start()
    for k in ks:
        greet({"task": task_peer(k)})
    for mask in range(1, groups):
        greet({"shard": flipped(mask)})
    second_load = load_both(1, 0, 1, first, first)
    top_loads = [load_both(k, 0, 1, 2 * first if k == 1 else 0, raw - (2 * first if k == 1 else 0)) for k in ks]
    deep_loads = [load_both(k, 1, layers - 1, 0, raw, columns - raw) for k in ks]
    own_sem = 1 + len(used)
    rest_loads = [load(delta_hbm, delta, k, 0, 1, raw, columns - raw, own_sem + k) for k in ks]
    own_load = load(delta_hbm, delta, 0, 0, layers, 0, columns, own_sem)

    @pl.when(is_hub)
    def _():
        for s in outside:
            greet({"shard": s})

    def masked(l, k, at):
        limit = limit_ref[l, expert]
        return jnp.where(score[k, l, :, at] < limit, delta[k, l, :, at].astype(F32), 0.0)

    def to_task(k, l, deep, c, n, recv):
        where = (k - 1, pl.ds(l, deep), slice(None), pl.ds(c, n))
        return remote(outgoing.at[where], incoming.at[where], send_sem, recv_sem.at[recv], {"task": task_peer(k)})

    raw_sends = [to_task(*unit, 0) for unit in raw_units]
    scaled_sends = [to_task(*unit, 1 + u // (2 * len(ks)) + u // (3 * len(ks))) for u, unit in enumerate(scaled_units)]
    hub_sends = jnp.logical_and(is_hub, me_task == 1)
    split = len(scaled_units) - 2
    legs = []
    if helpers:
        k, l, deep, c, n = scaled_units[split]
        skipped = detour * len(helpers)
        hub_copy = to_task(k, l, deep, c + skipped, n - skipped, 2)
        for j, s in enumerate(helpers):
            at = pl.ds(c + j * detour, detour)
            legs.append((
                remote(outgoing.at[0, l, :, at], detoured, send_sem, leg_sem, {"shard": s, "task": 0}),
                remote(detoured, incoming.at[0, l, :, at], load_sem.at[1], recv_sem.at[2], {"shard": HUB}),
            ))

    limit_copy.wait()
    early = 3
    held_back = jnp.logical_and(is_hub, tasks > 1)
    slow = jnp.logical_and(lax.rem(me_shard, 2) == 1, not_hub)
    for u, (k, l, deep, c, n) in enumerate(raw_units):
        ready = []
        if u == 0:
            ready = [first_load]
        elif u == 1:
            ready = [second_load]
        elif u == 2:
            ready = top_loads
        elif l:
            ready, deep_loads = deep_loads, []
        for copy in ready:
            copy.wait()
        for layer in range(l, l + deep):

            def prepare(at, layer=layer, k=k):
                outgoing[k - 1, layer, :, at] = masked(layer, k, at).astype(BF16)

            sweep(c, n, prepare)
        if u == 0:
            away = jnp.where(expert == HUB // groups, 0, 1)
            pl.semaphore_wait(barrier, tasks - 1 + groups - 1 + away)
        if u < 3:
            raw_sends[u].start()
        elif u < early:
            @pl.when(jnp.logical_not(slow))
            def _(u=u):
                raw_sends[u].start()
        else:
            @pl.when(lax.rem(me_shard, 2) == 0)
            def _(u=u):
                raw_sends[u].start()

    score_loads = [load(score_hbm, score, k, 0, layers, raw, columns - raw, 1 + k) for k in ks]
    own_score_load = load(score_hbm, score, 0, 0, layers, 0, columns, 1)
    for copy in rest_loads:
        copy.wait()
    own_load.wait()
    for k in range(tasks):
        for l in range(layers):

            def add_up(at, l=l, k=k):
                size = jnp.abs(delta[k, l, :, at].astype(F32))
                sums[k, l : l + 1, at] = jnp.sum(size, axis=0, keepdims=True)

            sweep(0, columns, add_up)
    total = jnp.zeros((layers, 128), F32)
    step = min(2048, columns)
    for k in range(tasks):

        def gather(i, carry, k=k):
            block = sums[k, :, pl.ds(pl.multiple_of(i * step, 128), step)]
            for j in range(step // 128):
                carry = carry + block[:, j * 128 : (j + 1) * 128]
            return carry

        total = lax.fori_loop(0, columns // step, gather, total)
    part[...] = total
    for u in range(3, len(raw_units)):
        @pl.when(slow)
        def _(u=u):
            raw_sends[u].start()


    slot = lax.rem(me_shard + (shards - 1 - HUB), shards)
    to_hub = remote(part, part_in.at[slot], load_sem.at[own_sem], hub_sem, {"shard": HUB})
    to_all = [remote(total_ref, total_ref, load_sem.at[own_sem], hub_sem, {"shard": s}) for s in others]
    all_parts = remote(
        part_in.at[pl.ds(0, shards - 1)], part_in.at[pl.ds(0, shards - 1)], load_sem.at[own_sem], hub_sem, {"shard": HUB}
    )

    @pl.when(not_hub)
    def _():
        to_hub.start()

    for m in range(1, groups):
        remote(sums, sums_in.at[m - 1], load_sem.at[0], sums_sem, {"shard": flipped(m)}).start()
    if groups > 1:
        pair_wait = remote(sums_in, sums_in, load_sem.at[0], sums_sem, {"shard": HUB})
        pair_wait.wait_send()
        pair_wait.wait_recv()

    for u in range(early, len(raw_units)):
        @pl.when(held_back)
        def _(u=u):
            raw_sends[u].start()

    for k in range(tasks):

        def join(at, k=k):
            value = sums[k, :, at]
            for m in range(groups - 1):
                value = value + sums_in[m, k, :, at]
            sums[k, :, at] = value

        sweep(0, columns, join)

    @pl.when(is_hub)
    def _():
        all_parts.wait_recv()
        value = part[...]
        for s in range(shards - 1):
            value = value + part_in[s]
        total_ref[...] = value
        for copy in to_all:
            copy.start()

    @pl.when(not_hub)
    def _():
        to_all[0].wait_recv()

    total = total_ref[...]
    grand_mean = jnp.sum(total, axis=1, keepdims=True) / (EXPERTS * row_total * width)

    def keep(k, at):
        mean = sums[k, :, at] / row_total
        return (0.2 + 0.7 * mean / (mean + grand_mean)).astype(BF16)

    segment = raw // groups
    mine = pl.ds(pl.multiple_of(lax.rem(me_shard, groups) * segment, 128), segment)
    for k in ks:

        def fill(at, k=k):
            chance[k - 1, :, at] = keep(k, at)

        sweep(0, raw, fill)

        def invert_out(at, k=k):
            out_rate[k - 1, :, at] = 1.0 / keep(k, at).astype(F32)

        sweep(raw, columns - raw, invert_out)
        remote(
            chance.at[k - 1, :, mine], chance_in.at[k - 1, :, mine], load_sem.at[0], chance_sem.at[0],
            {"task": task_peer(k)},
        ).start()

    for copy in score_loads:
        copy.wait()
    for u, (k, l, deep, c, n) in enumerate(scaled_units):
        for layer in range(l, l + deep):

            def rescale(at, layer=layer, k=k):
                value = masked(layer, k, at) * out_rate[k - 1, layer : layer + 1, at]
                held = jnp.clip(value, -BF16_MAX, BF16_MAX)
                outgoing[k - 1, layer, :, at] = jnp.where(jnp.abs(value) <= F32_MAX, held, value).astype(BF16)

            sweep(c, n, rescale)
        if helpers and u == split:
            @pl.when(hub_sends)
            def _():
                for there, _ in legs:
                    there.start()

            @pl.when(jnp.logical_not(hub_sends))
            def _():
                scaled_sends[split].start()
        else:
            @pl.when(jnp.logical_not(hub_sends))
            def _(u=u):
                scaled_sends[u].start()

    own_score_load.wait()

    def invert_own(at):
        own_rate[:, at] = 1.0 / keep(0, at).astype(F32)

    sweep(0, columns, invert_own)
    for l in range(layers):

        def hold(at, l=l):
            own[l, :, at] = masked(l, 0, at) * own_rate[l : l + 1, at]

        sweep(0, columns, hold)

    if ks:
        got = chance_in.at[:, :, mine]
        remote(got, got, load_sem.at[0], chance_sem.at[0], {"shard": HUB}).wait_recv()
        for k in ks:
            for mask in range(1, groups):
                piece = chance_in.at[k - 1, :, mine]
                remote(piece, piece, load_sem.at[0], chance_sem.at[1], {"shard": flipped(mask)}).start()
        if groups > 1:
            shared = chance_in.at[:, :, pl.ds(0, segment * (groups - 1))]
            remote(shared, shared, load_sem.at[0], chance_sem.at[1], {"shard": HUB}).wait_recv()
    for k in ks:

        def invert_in(at, k=k):
            in_rate[k - 1, :, at] = 1.0 / chance_in[k - 1, :, at].astype(F32)

        sweep(0, raw, invert_in)

    def arrived(recv, l, deep, c, n):
        piece = incoming.at[:, pl.ds(l, deep), :, pl.ds(c, n)]
        remote(piece, piece, send_sem, recv_sem.at[recv], {"shard": HUB}).wait_recv()

    def combine(l, deep, c, n, scaled):
        for layer in range(l, l + deep):

            def add(at, layer=layer):
                total = own[layer, :, at]
                for k in ks:
                    value = incoming[k - 1, layer, :, at].astype(F32)
                    if not scaled:
                        value = value * in_rate[k - 1, layer : layer + 1, at]
                    total = total + value
                merged[layer, :, at] = total.astype(BF16)

            sweep(c, n, add)

    arrived(0, 0, layers, 0, raw)
    combine(0, layers, 0, raw, False)

    @pl.when(hub_sends)
    def _():
        for u, copy in enumerate(scaled_sends):
            if helpers and u == split:
                hub_copy.start()
            else:
                copy.start()

    for j, s in enumerate(helpers):
        @pl.when(jnp.logical_and(me_shard == s, me_task == 0))
        def _(j=j):
            legs[j][0].wait_recv()
            legs[j][1].start()

    arrived(1, 0, layers - 1, raw, columns - raw)
    combine(0, layers - 1, raw, columns - raw, True)
    arrived(2, layers - 1, 1, raw, cut - raw)
    combine(layers - 1, 1, raw, cut - raw, True)
    remote(chance_in, chance_in, load_sem.at[0], chance_sem.at[0], {"shard": HUB}).wait_send()

    @pl.when(is_hub)
    def _():
        all_parts.wait_send()

    @pl.when(not_hub)
    def _():
        to_hub.wait_send()

    for j, s in enumerate(helpers):
        @pl.when(jnp.logical_and(me_shard == s, me_task == 0))
        def _(j=j):
            legs[j][1].wait_send()

    arrived(3, layers - 1, 1, cut, columns - cut)
    combine(layers - 1, 1, cut, columns - cut, True)
    remote(outgoing, outgoing, send_sem, recv_sem.at[0], {"shard": HUB}).wait_send()


def put_out(value, out_hbm, sem):
    copy = pltpu.make_async_copy(value, out_hbm, sem)
    copy.start()
    copy.wait()


def on_device(task_deltas, rank_scores, keep_limits):
    tasks, shards = lax.axis_size("task"), lax.axis_size("shard")
    _, layers, rows, width = task_deltas.shape
    columns = width // tasks
    others = tasks - 1
    groups = shards // EXPERTS
    raw, _, _, _, _ = plan(layers, columns, tasks, groups)
    _, detour = detours(layers, columns, tasks, shards, groups)
    dma = pltpu.SemaphoreType.DMA
    keep_limits = pltpu.with_memory_space_constraint(keep_limits, pltpu.HBM)
    result = pl.pallas_call(
        functools.partial(kernel, (layers, rows, width, tasks, shards)),
        out_shape=jax.ShapeDtypeStruct((layers, rows, columns), BF16),
        in_specs=[
            pl.BlockSpec(memory_space=pltpu.HBM),
            pl.BlockSpec(memory_space=pltpu.HBM),
            pl.BlockSpec(memory_space=pltpu.HBM),
        ],
        out_specs=pl.BlockSpec(memory_space=pltpu.VMEM),
        scratch_shapes=[
            pltpu.SMEM(keep_limits.shape[1:], jnp.int32),
            pltpu.VMEM((tasks, layers, rows, columns), BF16),
            pltpu.VMEM((tasks, layers, rows, columns), jnp.int32),
            pltpu.VMEM((others, layers, rows, columns), BF16),
            pltpu.VMEM((others, layers, rows, columns), BF16),
            pltpu.VMEM((tasks, layers, columns), F32),
            pltpu.VMEM((max(groups - 1, 1), tasks, layers, columns), F32),
            pltpu.VMEM((layers, 128), F32),
            pltpu.VMEM((shards - 1, layers, 128), F32),
            pltpu.VMEM((layers, 128), F32),
            pltpu.VMEM((others, layers, raw), BF16),
            pltpu.VMEM((others, layers, raw), BF16),
            pltpu.VMEM((layers, columns), F32),
            pltpu.VMEM((others, layers, columns), F32),
            pltpu.VMEM((others, layers, raw), F32),
            pltpu.VMEM((layers, rows, columns), F32),
            pltpu.VMEM((rows, max(detour, 128)), BF16),
            dma((4 + 3 * others,)),
            dma(()),
            dma((4,)),
            dma(()),
            dma(()),
            dma((2,)),
            dma(()),
        ],
        compiler_params=pltpu.CompilerParams(
            collective_id=0, has_side_effects=True, vmem_limit_bytes=52 * 2**20
        ),
        name="merge",
    )(task_deltas, rank_scores, keep_limits)
    return pl.pallas_call(
        put_out,
        out_shape=jax.ShapeDtypeStruct(result.shape, result.dtype),
        in_specs=[pl.BlockSpec(memory_space=pltpu.VMEM)],
        out_specs=pl.BlockSpec(memory_space=pltpu.HBM),
        scratch_shapes=[dma(())],
        compiler_params=pltpu.CompilerParams(vmem_limit_bytes=4 * 2**20),
        name="put",
    )(result)


def solution(mesh):
    return jax.shard_map(
        on_device,
        mesh=mesh,
        in_specs=(
            P("task", None, "shard", None),
            P("task", None, "shard", None),
            P("task", None, None),
        ),
        out_specs=P(None, "shard", "task"),
        check_vma=False,
    )
```

```python
import functools
import jax
import jax.numpy as jnp
from jax import lax
from jax.experimental import pallas as pl
from jax.experimental.pallas import tpu as pltpu
from jax.sharding import PartitionSpec as P

EXPERTS = 8
F32 = jnp.float32
BF16 = jnp.bfloat16
MESH = pl.DeviceIdType.MESH
BF16_MAX = float(jnp.finfo(BF16).max)
F32_MAX = float(jnp.finfo(F32).max)
HUB = 1


def plan(layers, columns, tasks, groups):
    unit = 128 * groups
    raw = columns // 2 // unit * unit
    first = min(512, raw // 4 // 128 * 128)
    last = min(1024, (columns - raw) // 4 // 128 * 128)
    cut = columns - last
    ks = range(1, tasks)
    raw_units = [(1, 0, 1, 0, first), (1, 0, 1, first, first), (1, 0, 1, 2 * first, raw - 2 * first)]
    raw_units += [(k, 0, 1, 0, raw) for k in ks if k > 1]
    raw_units += [(k, 1, layers - 1, 0, raw) for k in ks]
    scaled_units = [(k, 0, 1, raw, columns - raw) for k in ks]
    scaled_units += [(k, 1, layers - 2, raw, columns - raw) for k in ks]
    scaled_units += [(k, layers - 1, 1, raw, cut - raw) for k in ks]
    scaled_units += [(k, layers - 1, 1, cut, last) for k in ks]
    return raw, first, cut, raw_units, scaled_units


def detours(layers, columns, tasks, shards, groups):
    helpers = list(range(HUB + groups, shards, groups)) if tasks == 2 else []
    if not helpers:
        return [], 0
    room = plan(layers, columns, tasks, groups)[4][-2][4]
    piece = min(columns * 3 // 64, room * 7 // 8 // len(helpers)) // 128 * 128
    return (helpers, piece) if piece else ([], 0)


def kernel(
    sizes, delta_hbm, score_hbm, limit_hbm, merged,
    limit_ref, delta, score, outgoing, incoming, sums, sums_in, part, part_in, total_ref,
    chance, chance_in, own_rate, out_rate, in_rate, own, detoured,
    load_sem, send_sem, recv_sem, sums_sem, hub_sem, chance_sem, leg_sem,
):
    layers, rows, width, tasks, shards = sizes
    columns = width // tasks
    groups = shards // EXPERTS
    all_bits = shards.bit_length() - 1
    raw, first, cut, raw_units, scaled_units = plan(layers, columns, tasks, groups)
    ks = list(range(1, tasks))
    me_shard, me_task = lax.axis_index("shard"), lax.axis_index("task")
    expert = me_shard // groups
    row_total = rows * groups
    is_hub = me_shard == HUB
    not_hub = jnp.logical_not(is_hub)
    others = [s for s in range(shards) if s != HUB]
    outside = [s for s in others if s // groups != HUB // groups]
    helpers, detour = detours(layers, columns, tasks, shards, groups)

    def flipped(mask):
        index = me_shard
        for bit in range(all_bits):
            stride = 2**bit
            if mask & stride:
                index = index + stride * (1 - 2 * lax.rem(me_shard // stride, 2))
        return index

    def task_peer(k):
        return lax.rem(me_task + k, tasks)

    def remote(src, dst, send, recv, where):
        return pltpu.make_async_remote_copy(
            src_ref=src, dst_ref=dst, send_sem=send, recv_sem=recv, device_id=where, device_id_type=MESH
        )

    def sweep(start, length, body):
        step = length
        while step > 2048:
            step //= 2
        if step % 128:
            step = 128

        def turn(i, carry):
            body(pl.ds(pl.multiple_of(start + i * step, 128), step))
            return carry

        if length == step:
            body(pl.ds(start, length))
        else:
            lax.fori_loop(0, length // step, turn, 0)

    barrier = pltpu.get_barrier_semaphore()

    def greet(where):
        pl.semaphore_signal(barrier, inc=1, device_id=where, device_id_type=MESH)

    used = []

    def load(whole, held, k, l, deep, c, n, sem):
        there = pl.ds(pl.multiple_of(task_peer(k) * columns + c, 128), n)
        copy = pltpu.make_async_copy(
            whole.at[0, pl.ds(l, deep), :, there], held.at[k, pl.ds(l, deep), :, pl.ds(c, n)], load_sem.at[sem]
        )
        copy.start()
        return copy

    def load_both(k, l, deep, c, n, more=0):
        sem = 1 + len(used)
        load(score_hbm, score, k, l, deep, c, n, sem)
        load(delta_hbm, delta, k, l, deep, c, n + more, sem)
        both = pl.ds(0, n + (n + more) // 2)
        used.append(pltpu.make_async_copy(
            score_hbm.at[0, pl.ds(l, deep), :, both], score.at[k, pl.ds(l, deep), :, both], load_sem.at[sem]
        ))
        return used[-1]

    first_load = load_both(1, 0, 1, 0, first)
    limit_copy = pltpu.make_async_copy(limit_hbm.at[0], limit_ref, load_sem.at[0])
    limit_copy.start()
    for k in ks:
        greet({"task": task_peer(k)})
    for mask in range(1, groups):
        greet({"shard": flipped(mask)})
    second_load = load_both(1, 0, 1, first, first)
    top_loads = [load_both(k, 0, 1, 2 * first if k == 1 else 0, raw - (2 * first if k == 1 else 0)) for k in ks]
    deep_loads = [load_both(k, 1, layers - 1, 0, raw, columns - raw) for k in ks]
    own_sem = 1 + len(used)
    rest_loads = [load(delta_hbm, delta, k, 0, 1, raw, columns - raw, own_sem + k) for k in ks]
    own_load = load(delta_hbm, delta, 0, 0, layers, 0, columns, own_sem)

    @pl.when(is_hub)
    def _():
        for s in outside:
            greet({"shard": s})

    def masked(l, k, at):
        limit = limit_ref[l, expert]
        return jnp.where(score[k, l, :, at] < limit, delta[k, l, :, at].astype(F32), 0.0)

    def to_task(k, l, deep, c, n, recv):
        where = (k - 1, pl.ds(l, deep), slice(None), pl.ds(c, n))
        return remote(outgoing.at[where], incoming.at[where], send_sem, recv_sem.at[recv], {"task": task_peer(k)})

    raw_sends = [to_task(*unit, 0) for unit in raw_units]
    scaled_sends = [to_task(*unit, 1 + u // (2 * len(ks)) + u // (3 * len(ks))) for u, unit in enumerate(scaled_units)]
    hub_sends = jnp.logical_and(is_hub, me_task == 1)
    split = len(scaled_units) - 2
    last_core = jnp.logical_and(lax.rem(me_shard, 2) == 1, me_task == tasks - 1)
    mid_core = jnp.logical_and(last_core, jnp.logical_not(hub_sends))
    legs = []
    if helpers:
        k, l, deep, c, n = scaled_units[split]
        skipped = detour * len(helpers)
        hub_copy = to_task(k, l, deep, c + skipped, n - skipped, 2)
        for j, s in enumerate(helpers):
            at = pl.ds(c + j * detour, detour)
            legs.append((
                remote(outgoing.at[0, l, :, at], detoured, send_sem, leg_sem, {"shard": s, "task": 0}),
                remote(detoured, incoming.at[0, l, :, at], load_sem.at[1], recv_sem.at[2], {"shard": HUB}),
            ))

    limit_copy.wait()
    early = 3
    held_back = jnp.logical_and(is_hub, tasks > 1)
    slow = jnp.logical_and(lax.rem(me_shard, 2) == 1, not_hub)
    for u, (k, l, deep, c, n) in enumerate(raw_units):
        ready = []
        if u == 0:
            ready = [first_load]
        elif u == 1:
            ready = [second_load]
        elif u == 2:
            ready = top_loads
        elif l:
            ready, deep_loads = deep_loads, []
        for copy in ready:
            copy.wait()
        for layer in range(l, l + deep):

            def prepare(at, layer=layer, k=k):
                outgoing[k - 1, layer, :, at] = masked(layer, k, at).astype(BF16)

            sweep(c, n, prepare)
        if u == 0:
            away = jnp.where(expert == HUB // groups, 0, 1)
            pl.semaphore_wait(barrier, tasks - 1 + groups - 1 + away)
        if u < 3:
            raw_sends[u].start()
        elif u < early:
            @pl.when(jnp.logical_not(slow))
            def _(u=u):
                raw_sends[u].start()
        else:
            @pl.when(lax.rem(me_shard, 2) == 0)
            def _(u=u):
                raw_sends[u].start()

    score_loads = [load(score_hbm, score, k, 0, layers, raw, columns - raw, 1 + k) for k in ks]
    own_score_load = load(score_hbm, score, 0, 0, layers, 0, columns, 1)
    for copy in rest_loads:
        copy.wait()
    own_load.wait()
    for k in range(tasks):
        for l in range(layers):

            def add_up(at, l=l, k=k):
                size = jnp.abs(delta[k, l, :, at].astype(F32))
                sums[k, l : l + 1, at] = jnp.sum(size, axis=0, keepdims=True)

            sweep(0, columns, add_up)
    total = jnp.zeros((layers, 128), F32)
    step = min(2048, columns)
    for k in range(tasks):

        def gather(i, carry, k=k):
            block = sums[k, :, pl.ds(pl.multiple_of(i * step, 128), step)]
            for j in range(step // 128):
                carry = carry + block[:, j * 128 : (j + 1) * 128]
            return carry

        total = lax.fori_loop(0, columns // step, gather, total)
    part[...] = total
    for u in range(3, len(raw_units)):
        @pl.when(slow)
        def _(u=u):
            raw_sends[u].start()


    slot = lax.rem(me_shard + (shards - 1 - HUB), shards)
    to_hub = remote(part, part_in.at[slot], load_sem.at[own_sem], hub_sem, {"shard": HUB})
    to_all = [remote(total_ref, total_ref, load_sem.at[own_sem], hub_sem, {"shard": s}) for s in others]
    all_parts = remote(
        part_in.at[pl.ds(0, shards - 1)], part_in.at[pl.ds(0, shards - 1)], load_sem.at[own_sem], hub_sem, {"shard": HUB}
    )

    @pl.when(not_hub)
    def _():
        to_hub.start()

    for m in range(1, groups):
        remote(sums, sums_in.at[m - 1], load_sem.at[0], sums_sem, {"shard": flipped(m)}).start()
    if groups > 1:
        pair_wait = remote(sums_in, sums_in, load_sem.at[0], sums_sem, {"shard": HUB})
        pair_wait.wait_send()
        pair_wait.wait_recv()

    for u in range(early, len(raw_units)):
        @pl.when(held_back)
        def _(u=u):
            raw_sends[u].start()

    for k in range(tasks):

        def join(at, k=k):
            value = sums[k, :, at]
            for m in range(groups - 1):
                value = value + sums_in[m, k, :, at]
            sums[k, :, at] = value

        sweep(0, columns, join)

    @pl.when(is_hub)
    def _():
        all_parts.wait_recv()
        value = part[...]
        for s in range(shards - 1):
            value = value + part_in[s]
        total_ref[...] = value
        for copy in to_all:
            copy.start()

    @pl.when(not_hub)
    def _():
        to_all[0].wait_recv()

    total = total_ref[...]
    grand_mean = jnp.sum(total, axis=1, keepdims=True) / (EXPERTS * row_total * width)

    def keep(k, at):
        mean = sums[k, :, at] / row_total
        return (0.2 + 0.7 * mean / (mean + grand_mean)).astype(BF16)

    segment = raw // groups
    mine = pl.ds(pl.multiple_of(lax.rem(me_shard, groups) * segment, 128), segment)
    for k in ks:

        def fill(at, k=k):
            chance[k - 1, :, at] = keep(k, at)

        sweep(0, raw, fill)

        def invert_out(at, k=k):
            out_rate[k - 1, :, at] = 1.0 / keep(k, at).astype(F32)

        sweep(raw, columns - raw, invert_out)
        remote(
            chance.at[k - 1, :, mine], chance_in.at[k - 1, :, mine], load_sem.at[0], chance_sem.at[0],
            {"task": task_peer(k)},
        ).start()

    for copy in score_loads:
        copy.wait()
    for u, (k, l, deep, c, n) in enumerate(scaled_units):
        for layer in range(l, l + deep):

            def rescale(at, layer=layer, k=k):
                value = masked(layer, k, at) * out_rate[k - 1, layer : layer + 1, at]
                held = jnp.clip(value, -BF16_MAX, BF16_MAX)
                outgoing[k - 1, layer, :, at] = jnp.where(jnp.abs(value) <= F32_MAX, held, value).astype(BF16)

            sweep(c, n, rescale)
        if helpers and u == split:
            @pl.when(hub_sends)
            def _():
                for there, _ in legs:
                    there.start()

            @pl.when(jnp.logical_not(last_core))
            def _():
                scaled_sends[split].start()
        else:
            @pl.when(jnp.logical_not(last_core))
            def _(u=u):
                scaled_sends[u].start()

    own_score_load.wait()

    def invert_own(at):
        own_rate[:, at] = 1.0 / keep(0, at).astype(F32)

    sweep(0, columns, invert_own)
    for l in range(layers):

        def hold(at, l=l):
            own[l, :, at] = masked(l, 0, at) * own_rate[l : l + 1, at]

        sweep(0, columns, hold)

    @pl.when(mid_core)
    def _():
        for copy in scaled_sends:
            copy.start()

    if ks:
        got = chance_in.at[:, :, mine]
        remote(got, got, load_sem.at[0], chance_sem.at[0], {"shard": HUB}).wait_recv()
        for k in ks:
            for mask in range(1, groups):
                piece = chance_in.at[k - 1, :, mine]
                remote(piece, piece, load_sem.at[0], chance_sem.at[1], {"shard": flipped(mask)}).start()
        if groups > 1:
            shared = chance_in.at[:, :, pl.ds(0, segment * (groups - 1))]
            remote(shared, shared, load_sem.at[0], chance_sem.at[1], {"shard": HUB}).wait_recv()
    for k in ks:

        def invert_in(at, k=k):
            in_rate[k - 1, :, at] = 1.0 / chance_in[k - 1, :, at].astype(F32)

        sweep(0, raw, invert_in)

    def arrived(recv, l, deep, c, n):
        piece = incoming.at[:, pl.ds(l, deep), :, pl.ds(c, n)]
        remote(piece, piece, send_sem, recv_sem.at[recv], {"shard": HUB}).wait_recv()

    def combine(l, deep, c, n, scaled):
        for layer in range(l, l + deep):

            def add(at, layer=layer):
                total = own[layer, :, at]
                for k in ks:
                    value = incoming[k - 1, layer, :, at].astype(F32)
                    if not scaled:
                        value = value * in_rate[k - 1, layer : layer + 1, at]
                    total = total + value
                merged[layer, :, at] = total.astype(BF16)

            sweep(c, n, add)

    arrived(0, 0, layers, 0, raw)
    combine(0, layers, 0, raw, False)

    @pl.when(hub_sends)
    def _():
        for u, copy in enumerate(scaled_sends):
            if helpers and u == split:
                hub_copy.start()
            else:
                copy.start()

    for j, s in enumerate(helpers):
        @pl.when(jnp.logical_and(me_shard == s, me_task == 0))
        def _(j=j):
            legs[j][0].wait_recv()
            legs[j][1].start()

    arrived(1, 0, layers - 1, raw, columns - raw)
    combine(0, layers - 1, raw, columns - raw, True)
    arrived(2, layers - 1, 1, raw, cut - raw)
    combine(layers - 1, 1, raw, cut - raw, True)
    remote(chance_in, chance_in, load_sem.at[0], chance_sem.at[0], {"shard": HUB}).wait_send()

    @pl.when(is_hub)
    def _():
        all_parts.wait_send()

    @pl.when(not_hub)
    def _():
        to_hub.wait_send()

    for j, s in enumerate(helpers):
        @pl.when(jnp.logical_and(me_shard == s, me_task == 0))
        def _(j=j):
            legs[j][1].wait_send()

    arrived(3, layers - 1, 1, cut, columns - cut)
    combine(layers - 1, 1, cut, columns - cut, True)
    remote(outgoing, outgoing, send_sem, recv_sem.at[0], {"shard": HUB}).wait_send()


def put_out(value, out_hbm, sem):
    copy = pltpu.make_async_copy(value, out_hbm, sem)
    copy.start()
    copy.wait()


def on_device(task_deltas, rank_scores, keep_limits):
    tasks, shards = lax.axis_size("task"), lax.axis_size("shard")
    _, layers, rows, width = task_deltas.shape
    columns = width // tasks
    others = tasks - 1
    groups = shards // EXPERTS
    raw, _, _, _, _ = plan(layers, columns, tasks, groups)
    _, detour = detours(layers, columns, tasks, shards, groups)
    dma = pltpu.SemaphoreType.DMA
    keep_limits = pltpu.with_memory_space_constraint(keep_limits, pltpu.HBM)
    result = pl.pallas_call(
        functools.partial(kernel, (layers, rows, width, tasks, shards)),
        out_shape=jax.ShapeDtypeStruct((layers, rows, columns), BF16),
        in_specs=[
            pl.BlockSpec(memory_space=pltpu.HBM),
            pl.BlockSpec(memory_space=pltpu.HBM),
            pl.BlockSpec(memory_space=pltpu.HBM),
        ],
        out_specs=pl.BlockSpec(memory_space=pltpu.VMEM),
        scratch_shapes=[
            pltpu.SMEM(keep_limits.shape[1:], jnp.int32),
            pltpu.VMEM((tasks, layers, rows, columns), BF16),
            pltpu.VMEM((tasks, layers, rows, columns), jnp.int32),
            pltpu.VMEM((others, layers, rows, columns), BF16),
            pltpu.VMEM((others, layers, rows, columns), BF16),
            pltpu.VMEM((tasks, layers, columns), F32),
            pltpu.VMEM((max(groups - 1, 1), tasks, layers, columns), F32),
            pltpu.VMEM((layers, 128), F32),
            pltpu.VMEM((shards - 1, layers, 128), F32),
            pltpu.VMEM((layers, 128), F32),
            pltpu.VMEM((others, layers, raw), BF16),
            pltpu.VMEM((others, layers, raw), BF16),
            pltpu.VMEM((layers, columns), F32),
            pltpu.VMEM((others, layers, columns), F32),
            pltpu.VMEM((others, layers, raw), F32),
            pltpu.VMEM((layers, rows, columns), F32),
            pltpu.VMEM((rows, max(detour, 128)), BF16),
            dma((4 + 3 * others,)),
            dma(()),
            dma((4,)),
            dma(()),
            dma(()),
            dma((2,)),
            dma(()),
        ],
        compiler_params=pltpu.CompilerParams(
            collective_id=0, has_side_effects=True, vmem_limit_bytes=52 * 2**20
        ),
        name="merge",
    )(task_deltas, rank_scores, keep_limits)
    return pl.pallas_call(
        put_out,
        out_shape=jax.ShapeDtypeStruct(result.shape, result.dtype),
        in_specs=[pl.BlockSpec(memory_space=pltpu.VMEM)],
        out_specs=pl.BlockSpec(memory_space=pltpu.HBM),
        scratch_shapes=[dma(())],
        compiler_params=pltpu.CompilerParams(vmem_limit_bytes=4 * 2**20),
        name="put",
    )(result)


def solution(mesh):
    return jax.shard_map(
        on_device,
        mesh=mesh,
        in_specs=(
            P("task", None, "shard", None),
            P("task", None, "shard", None),
            P("task", None, None),
        ),
        out_specs=P(None, "shard", "task"),
        check_vma=False,
    )
```
